128 devices in a mesh: row: 8 (over x, core), col: 16 (over z, y).
Axes of the slice: x: 4, y: 4, z: 4, core: 2. Of those that a mesh axis runs over, the one named last changes fastest.
Arguments:
- rhs: float32 [32, 1048576], P(None, ('row', 'col')), may hold values from -12.5 to 12.5
- near_blocks: bfloat16 [16384, 4, 4096], P(('row', 'col')), may hold values from -0.1875 to 0.1875
- near_offsets: int32 [16384, 4], P(('row', 'col')), may hold values from -4 to 4, as said below
- v_factor: bfloat16 [16384, 2048], P(('row', 'col')), may hold values from -0.75 to 0.75
- mix_col: bfloat16 [8, 128, 512, 512], P('row', 'col'), may hold values from -0.25 to 0.25
- mix_row: bfloat16 [8, 256, 256, 256], P('row', 'col'), may hold values from -0.375 to 0.375
- u_factor: bfloat16 [16384, 2048], P(('row', 'col')), may hold values from -0.75 to 0.75
Outputs:
- solution: float32 [32, 1048576], P(None, ('row', 'col'))
- residual: float32 [32, 1048576], P(None, ('row', 'col'))
The draws below stay inside these ranges and needn't reach their ends.
Inputs may be any that keep to these rules, and one draw needn't show every extreme that they name: `near_offsets`: column 0 is 0; the other entries of a row are distinct and nonzero. In every aligned block of 128 rows some row holds -4 and some row holds 4.
All inputs are finite; a program needn't handle non-finite values.
Results may differ from the reference program's by a relative error of at most 0.0054.
Values may be sent and summed in bfloat16 or wider, within the bound.
No kernel may reach another device: no remote copies, remote signals or barrier semaphores. Data moves between devices by JAX's collectives and lax.ppermute only.
A program may use at most 128 MiB of HBM per device.

```python
import jax
import jax.numpy as jnp
from jax import lax

RHS = 32
LEAF = 64
RANK = 32
NNEAR = 4
HALO = 4
LEAVES_DEV = 128
NLEAVES = 16384
N_UNKNOWNS = 1048576
SLOTS = 8
SUBSLOTS = 1
N_ROW = 8
N_COL = 16
DEVICES = 128


def draw_rhs(key, part):
    scale_key = jax.random.fold_in(key, 11)
    value_key = jax.random.fold_in(key, 12)
    scales = jnp.exp(jax.random.uniform(scale_key, (DEVICES,), jnp.float32, jnp.log(0.2), jnp.log(2.5)))
    scales = jnp.repeat(scales, N_UNKNOWNS // DEVICES)[None, :]
    values = jnp.clip(jax.random.normal(value_key, (RHS, N_UNKNOWNS), jnp.float32), -5.0, 5.0)
    return (values * scales).astype(jnp.float32)


def draw_near_offsets(key, part):
    score_key = jax.random.fold_in(key, 21)
    choices_count = 2 * HALO
    column = jnp.arange(choices_count, dtype=jnp.int32)
    candidates = jnp.where(column < HALO, column - HALO, column - HALO + 1)
    scores = jax.random.randint(score_key, (NLEAVES, choices_count), 0, 2 ** 20, dtype=jnp.int32) * choices_count + column[None, :]
    leading = (jnp.arange(NLEAVES, dtype=jnp.int32) % LEAVES_DEV == 0)[:, None]
    forced = jnp.where(column == 0, -2, jnp.where(column == choices_count - 1, -1, scores))
    scores = jnp.where(leading, forced, scores)
    order = jnp.argsort(scores, axis=1)
    picked = candidates[order[:, :NNEAR - 1]]
    return jnp.concatenate([jnp.zeros((NLEAVES, 1), jnp.int32), picked.astype(jnp.int32)], axis=1)


def shard_levels(stream_key, dims, shards, low, largest):
    loudness = 1.0
    for axis_at, shards_of in shards:
        draws = jax.random.uniform(jax.random.fold_in(jax.random.fold_in(stream_key, 6), axis_at), (shards_of,), jnp.float32, low / len(shards), largest / len(shards))
        loudness = loudness * jnp.repeat(jnp.exp(draws), dims[axis_at] // shards_of).reshape((-1,) + (1,) * (len(dims) - 1 - axis_at))
    return loudness


def normal_values(rng, shape, scale, most, split=(), held_as=jnp.bfloat16):
    level = shard_levels(rng, shape, split, -0.22, 0.18) if split else 1.0
    values = jax.random.normal(rng, shape, jnp.float32) * scale * level
    return jnp.minimum(jnp.maximum(values, -most), most).astype(held_as)


def setup_inputs(seed: int = 0) -> dict:
    arg_keys = jax.random.split(jax.random.key(seed), 8)
    rhs = draw_rhs(jax.random.fold_in(arg_keys[7], 71), 0)
    near_blocks = normal_values(arg_keys[1], (NLEAVES, NNEAR, LEAF * LEAF), (4 * NNEAR * LEAF) ** -0.5, 0.1875, ((0, 128),))
    near_offsets = draw_near_offsets(jax.random.fold_in(arg_keys[7], 71), 0)
    v_factor = normal_values(arg_keys[3], (NLEAVES, LEAF * RANK), LEAF ** -0.5, 0.75, ((0, 128),))
    mix_col = normal_values(arg_keys[4], (N_ROW, N_COL * SLOTS, N_COL * RANK, N_COL * RANK), (N_COL * RANK) ** -0.5, 0.25, ((0, 8), (1, 16)))
    mix_row = normal_values(arg_keys[5], (N_ROW * SUBSLOTS, N_COL * N_COL, N_ROW * RANK, N_ROW * RANK), (N_ROW * RANK) ** -0.5, 0.375, ((0, 8), (1, 16)))
    u_factor = normal_values(arg_keys[6], (NLEAVES, RANK * LEAF), (2 * RANK) ** -0.5, 0.75, ((0, 128),))
    return {"rhs": rhs, "near_blocks": near_blocks, "near_offsets": near_offsets, "v_factor": v_factor, "mix_col": mix_col, "mix_row": mix_row, "u_factor": u_factor}


def near_term(vector_bf, near_blocks, near_offsets):
    padded = jnp.pad(vector_bf, ((0, 0), (HALO * LEAF, HALO * LEAF)))
    padded = padded.reshape(RHS, NLEAVES + 2 * HALO, LEAF)
    blocks = near_blocks.reshape(DEVICES, LEAVES_DEV, NNEAR, LEAF, LEAF)
    offsets = near_offsets.reshape(DEVICES, LEAVES_DEV, NNEAR)

    def one_block(device):
        position = device * LEAVES_DEV + jnp.arange(LEAVES_DEV, dtype=jnp.int32)[:, None] + offsets[device] + HALO
        picked = padded[:, position, :].astype(jnp.float32)
        return jnp.einsum('slnu,lnvu->slv', picked, blocks[device].astype(jnp.float32))
    result = lax.map(one_block, jnp.arange(DEVICES, dtype=jnp.int32))
    return jnp.transpose(result, (1, 0, 2, 3)).reshape(RHS, N_UNKNOWNS)

def far_term(vector_bf, v_factor, mix_col, mix_row, u_factor):
    width_col = N_COL * RANK
    width_row = N_ROW * RANK
    local = vector_bf.reshape(RHS, NLEAVES, LEAF).astype(jnp.float32)
    factor = v_factor.reshape(NLEAVES, LEAF, RANK).astype(jnp.float32)
    coeffs = jnp.einsum('slu,luk->lsk', local, factor).astype(jnp.bfloat16)
    coeffs = coeffs.reshape(N_ROW, N_COL, N_COL, SLOTS, RHS, RANK)
    first_mix = mix_col.reshape(N_ROW, N_COL, SLOTS, N_COL, RANK, width_col)

    def level_one(rowgrp):
        return jnp.einsum('cgjsk,gjckm->gjsm', coeffs[rowgrp].astype(jnp.float32), first_mix[rowgrp].astype(jnp.float32)).astype(jnp.bfloat16)
    first = lax.map(level_one, jnp.arange(N_ROW, dtype=jnp.int32))
    first = first.reshape(N_ROW, N_COL, N_ROW, SUBSLOTS, RHS, N_COL, RANK)
    second_mix = mix_row.reshape(N_ROW, SUBSLOTS, N_COL, N_COL, N_ROW, RANK, width_row)
    expand = u_factor.reshape(N_ROW, N_COL, SUBSLOTS, N_COL, N_ROW, RANK, LEAF)

    def level_two(target):
        picked = lax.dynamic_index_in_dim(first, target, 2, keepdims=False)
        second = jnp.einsum('rgjspk,jgprkn->gjpsn', picked.astype(jnp.float32), second_mix[target].astype(jnp.float32)).astype(jnp.bfloat16)
        second = second.reshape(N_COL, SUBSLOTS, N_COL, RHS, N_ROW, RANK)
        out = jnp.einsum('gjpsqk,gjpqku->sgjpqu', second.astype(jnp.float32), expand[target].astype(jnp.float32))
        return out.reshape(RHS, N_COL * LEAVES_DEV * LEAF)
    result = lax.map(level_two, jnp.arange(N_ROW, dtype=jnp.int32))
    return jnp.transpose(result, (1, 0, 2)).reshape(RHS, N_UNKNOWNS)

def reference(rhs, near_blocks, near_offsets, v_factor, mix_col, mix_row, u_factor):

    def operator(vector):
        vector_bf = vector.astype(jnp.bfloat16)
        return vector + near_term(vector_bf, near_blocks, near_offsets) + far_term(vector_bf, v_factor, mix_col, mix_row, u_factor)
    rhs_length = jnp.sqrt(lax.optimization_barrier(jnp.sum(rhs * rhs, axis=1)))
    basis_first = rhs / rhs_length[:, None]
    image_first = operator(basis_first)
    h_one_one = lax.optimization_barrier(jnp.sum(basis_first * image_first, axis=1))
    rest_first = image_first - h_one_one[:, None] * basis_first
    h_two_one = jnp.sqrt(lax.optimization_barrier(jnp.sum(rest_first * rest_first, axis=1)))
    basis_second = rest_first / h_two_one[:, None]
    image_second = operator(basis_second)
    h_one_two = lax.optimization_barrier(jnp.sum(basis_first * image_second, axis=1))
    h_two_two = lax.optimization_barrier(jnp.sum(basis_second * image_second, axis=1))
    rest_second = image_second - h_one_two[:, None] * basis_first - h_two_two[:, None] * basis_second
    h_three_two = jnp.sqrt(lax.optimization_barrier(jnp.sum(rest_second * rest_second, axis=1)))
    m_first = h_one_one * h_one_one + h_two_one * h_two_one
    m_cross = h_one_one * h_one_two + h_two_one * h_two_two
    m_second = h_one_two * h_one_two + h_two_two * h_two_two + h_three_two * h_three_two
    determ = m_first * m_second - m_cross * m_cross
    coef_first = rhs_length * (m_second * h_one_one - m_cross * h_one_two) / determ
    coef_second = rhs_length * (m_first * h_one_two - m_cross * h_one_one) / determ
    solution = coef_first[:, None] * basis_first + coef_second[:, None] * basis_second
    residual = rhs - coef_first[:, None] * image_first - coef_second[:, None] * image_second
    return (solution, residual)
```

```python
import functools

import jax
import jax.numpy as jnp
from jax import lax
from jax.experimental import pallas as pl
from jax.experimental.pallas import tpu as pltpu
from jax.sharding import Mesh
from jax.sharding import PartitionSpec as P

LEAF = 64
RANK = 32
HALO = 4
RHS = 32
LANES = 128
ROW_COL = ("row_0", "row_1", "col_0", "col_1")
ROW = ("row_0", "row_1")
COL = ("col_0", "col_1")
F32 = jnp.float32
BF16 = jnp.bfloat16


def dot(a, b):
    return jnp.dot(a, b, preferred_element_type=F32)


def dot_t(a, b):
    return lax.dot_general(a, b, (((1,), (1,)), ((), ())), preferred_element_type=F32)


def lane_group(rows):
    return lax.broadcasted_iota(jnp.int32, (rows, LANES), 1) // RANK


def lane_half(rows):
    return lax.broadcasted_iota(jnp.int32, (rows, LANES), 1) < LEAF


def spread_v_kernel(rhs_ref, v_ref, turn_ref, vbd_ref, z_ref, low_ref, high_ref, scratch):
    group = lane_group(16)
    shift = turn_ref[0] * RANK
    groups = vbd_ref.shape[0]
    for g in range(groups):
        slot = g % scratch.shape[0]
        for leaf in range(4):
            x = v_ref[4 * g + leaf].astype(F32)
            for ur in range(4):
                turned = x if leaf == ur else pltpu.roll(x, (leaf - ur) * RANK % LANES, 1)
                scratch[slot, pl.ds(leaf * LEAF + ur, 16, stride=4), :] = jnp.where(group == leaf, turned, 0.0)
        vbd_ref[g] = scratch[slot].astype(BF16)
    for g in range(groups):
        part = dot(rhs_ref[:, 256 * g : 256 * (g + 1)].astype(BF16), vbd_ref[g])
        z_ref[g // 2, :, (g % 2) * LANES : (g % 2 + 1) * LANES] = pltpu.roll(part, shift, 1).astype(BF16)
    edge = HALO * LEAF
    low_ref[...] = rhs_ref[:, :edge].astype(BF16)
    high_ref[...] = rhs_ref[:, rhs_ref.shape[1] - edge :].astype(BF16)


def spread_near_kernel(near_ref, out_ref, rows, wide):
    half = lane_half(32)
    for leaf in range(near_ref.shape[0]):
        rows[leaf] = near_ref[leaf].astype(F32)
        for h in range(2):
            even = rows[leaf, pl.ds(2 * h, 32, stride=4), :]
            odd = rows[leaf, pl.ds(2 * h + 1, 32, stride=4), :]
            wide[leaf, h, pl.ds(0, 32, stride=2), :] = jnp.where(half, even, pltpu.roll(odd, LEAF, 1))
            wide[leaf, h, pl.ds(1, 32, stride=2), :] = jnp.where(half, pltpu.roll(even, LEAF, 1), odd)
            out_ref[leaf // 2, (leaf % 2) * LEAF : (leaf % 2 + 1) * LEAF, h * LANES : (h + 1) * LANES] = wide[leaf, h].astype(BF16)


def spread_u_kernel(u_ref, out_ref, scratch):
    half = lane_half(16)
    zero = jnp.zeros((RANK, LANES), F32)
    for g in range(out_ref.shape[0]):
        slot = g % scratch.shape[0]
        for leaf in range(4):
            x = u_ref[4 * g + leaf].astype(F32)
            other = pltpu.roll(x, LEAF, 1)
            tile = leaf // 2
            keep = half if leaf % 2 == 0 else ~half
            for kp in range(2):
                scratch[slot, tile, pl.ds(leaf * RANK + kp, 16, stride=2), :] = jnp.where(
                    keep, x if kp == leaf % 2 else other, 0.0
                )
            scratch[slot, 1 - tile, leaf * RANK : (leaf + 1) * RANK, :] = zero
        for tile in range(2):
            out_ref[g, :, tile * LANES : (tile + 1) * LANES] = scratch[slot, tile].astype(BF16)


def near_kernel(v_ref, low_ref, high_ref, place_ref, near_ref, out_ref, plain, swapped):
    half = lane_half(RHS)
    edge = HALO // 2
    tiles = v_ref.shape[1] // LANES

    def put(t, x):
        plain[t] = x.astype(BF16)
        swapped[t] = pltpu.roll(x, LEAF, 1).astype(BF16)

    for t in range(edge):
        put(t, low_ref[:, t * LANES : (t + 1) * LANES].astype(F32))
        put(edge + tiles + t, high_ref[:, t * LANES : (t + 1) * LANES].astype(F32))
    for t in range(tiles):
        put(edge + t, v_ref[:, t * LANES : (t + 1) * LANES])

    def pick(block, leaf, side):
        place = place_ref[block, leaf]
        tile = place // 2
        odd = place % 2
        x = jnp.where(odd == side, plain[tile].astype(F32), swapped[tile].astype(F32))
        return x

    def one(pair):
        rows = []
        for par in range(2):
            leaf = 2 * pair + par
            tiles_of = [
                jnp.where(half, pick(2 * h, leaf, 0), pick(2 * h + 1, leaf, 1)).astype(BF16)
                for h in range(2)
            ]
            rows.append(jnp.concatenate(tiles_of, axis=1))
        both = dot_t(jnp.concatenate(rows, axis=0), near_ref[pair])
        return jnp.where(half, both[:RHS], both[RHS:])

    for pair in range(near_ref.shape[0]):
        out_ref[:, pair * LANES : (pair + 1) * LANES] = one(pair)


def gather_lanes(parts, where_from, group):
    x = parts[(0 - where_from) % 4]
    for q in range(1, 4):
        x = jnp.where(group == q, parts[(q - where_from) % 4], x)
    return x


def turned_rows(ref_rows, count, where_from):
    order = [4 * four + (q - where_from) % 4 for four in range(count // 4) for q in range(4)]
    return jnp.concatenate([ref_rows[c * RANK : (c + 1) * RANK] for c in order], axis=0)


def first_mix_kernel(z_ref, mix_ref, turn_ref, out_ref):
    n_col = z_ref.shape[0]
    group = lane_group(RHS)
    shift = turn_ref[0] * RANK
    for j in range(mix_ref.shape[0]):
        tile = j // 4
        lhs = jnp.concatenate(
            [
                gather_lanes(
                    [z_ref[4 * four + c, :, tile * LANES : (tile + 1) * LANES] for c in range(4)], j % 4, group
                )
                for four in range(n_col // 4)
            ],
            axis=1,
        )
        out = dot(lhs, turned_rows(mix_ref[j], n_col, j % 4))
        for t in range(out.shape[1] // LANES):
            out_ref[j, :, t * LANES : (t + 1) * LANES] = pltpu.roll(
                out[:, t * LANES : (t + 1) * LANES], shift, 1
            ).astype(BF16)


def second_mix(t1_ref, mix_ref, t2_ref):
    n_row = t1_ref.shape[0]
    group = lane_group(RHS)
    for p in range(mix_ref.shape[0]):
        tile = p // 4
        lhs = jnp.concatenate(
            [
                gather_lanes(
                    [t1_ref[4 * four + r, :, tile * LANES : (tile + 1) * LANES] for r in range(4)], p % 4, group
                )
                for four in range(n_row // 4)
            ],
            axis=1,
        )
        t2_ref[p] = dot(lhs, turned_rows(mix_ref[p], n_row, p % 4)).astype(BF16)


def far_tile(t2_ref, ubd_ref, g):
    return dot(t2_ref[g // 2, :, (g % 2) * LANES : (g % 2 + 1) * LANES], ubd_ref[g])


def second_mix_kernel(t1_ref, mix_ref, ubd_ref, near_ref, vbd_ref, turn_ref, d_ref, z_ref, low_ref, high_ref, t2_ref):
    second_mix(t1_ref, mix_ref, t2_ref)
    shift = turn_ref[0] * RANK
    groups = ubd_ref.shape[0]
    for g in range(groups):
        lanes = slice(256 * g, 256 * (g + 1))
        d_ref[:, lanes] = far_tile(t2_ref, ubd_ref, g) + near_ref[:, lanes]
    for g in range(groups):
        lanes = slice(256 * g, 256 * (g + 1))
        part = dot(d_ref[:, lanes].astype(BF16), vbd_ref[g])
        z_ref[g // 2, :, (g % 2) * LANES : (g % 2 + 1) * LANES] = pltpu.roll(part, shift, 1).astype(BF16)
    edge = HALO * LEAF
    low_ref[...] = d_ref[:, :edge].astype(BF16)
    high_ref[...] = d_ref[:, d_ref.shape[1] - edge :].astype(BF16)


def last_mix_kernel(t1_ref, mix_ref, ubd_ref, near_ref, rhs_ref, d_ref, e_ref, sums_ref, t2_ref):
    second_mix(t1_ref, mix_ref, t2_ref)
    total = [jnp.zeros((RHS, LANES), F32) for _ in range(6)]
    for g in range(ubd_ref.shape[0]):
        wide = far_tile(t2_ref, ubd_ref, g) + near_ref[:, 256 * g : 256 * (g + 1)]
        e_ref[:, 256 * g : 256 * (g + 1)] = wide
        for t in range(2):
            lanes = slice(256 * g + LANES * t, 256 * g + LANES * (t + 1))
            r, d, e = rhs_ref[:, lanes], d_ref[:, lanes], wide[:, LANES * t : LANES * (t + 1)]
            terms = (r * r, r * d, d * d, r * e, d * e, e * e)
            total = [a + b for a, b in zip(total, terms)]
    stacked = jnp.concatenate(total + [jnp.zeros((2 * RHS, LANES), F32)], axis=0)
    row = jnp.sum(stacked.T, axis=0, keepdims=True)
    sums_ref[...] = jnp.broadcast_to(row, sums_ref.shape)


def finish_kernel(sums_ref, rhs_ref, d_ref, e_ref, solution_ref, residual_ref):
    row = jnp.sum(sums_ref[...], axis=0, keepdims=True)
    columns = jnp.broadcast_to(row, (LANES, row.shape[1])).T
    rr, rd, dd, re, de, ee = [columns[i * RHS : (i + 1) * RHS] for i in range(6)]
    scale = 1.0 / rr
    alpha = rd * scale
    h21_sq = (dd - alpha * rd) * scale
    h11 = 1.0 + alpha
    cross = re * scale - alpha * alpha
    inverse = 1.0 / h21_sq
    gain = ((de - alpha * dd - alpha * re + alpha * (alpha * rd)) * scale) * inverse
    h22 = 1.0 + gain
    spread = ((ee - 2.0 * alpha * de + alpha * (alpha * dd)) * scale) * inverse
    h32_sq = spread - gain * gain - cross * (cross * inverse)
    minor = h11 * h22 - cross
    determ = minor * minor + h32_sq * (h11 * h11 + h21_sq)
    x_first = (h22 * minor + h11 * h32_sq) / determ
    x_second = -minor / determ
    on_rhs = x_first - alpha * x_second
    on_d = x_first + x_second * (1.0 - alpha)
    for t in range(rhs_ref.shape[1] // LANES):
        lanes = slice(t * LANES, (t + 1) * LANES)
        r, d, e = rhs_ref[:, lanes], d_ref[:, lanes], e_ref[:, lanes]
        solution_ref[:, lanes] = on_rhs * r + x_second * d
        residual_ref[:, lanes] = (1.0 - on_rhs) * r - on_d * d - x_second * e


VMEM = pl.BlockSpec(memory_space=pltpu.VMEM)
SMEM = pl.BlockSpec(memory_space=pltpu.SMEM)


def shape(dims, dtype):
    return jax.ShapeDtypeStruct(dims, dtype)


def call(kernel, in_specs, outs, scratch=(), flops=1_000_000, **more):
    out_specs = jax.tree.map(lambda _: VMEM, outs)
    return pl.pallas_call(
        kernel,
        in_specs=in_specs,
        out_shape=outs,
        out_specs=more.pop("out_specs", out_specs),
        scratch_shapes=list(scratch),
        cost_estimate=pl.CostEstimate(flops=flops, bytes_accessed=1_000_000, transcendentals=0),
        name=kernel.__name__,
        **more,
    )


def body(rhs, near_blocks, near_offsets, v_factor, mix_col, mix_row, u_factor):
    count = rhs.shape[1]
    leaves = near_offsets.shape[0]
    n_row = lax.axis_size(ROW)
    n_col = lax.axis_size(COL)
    devices = n_row * n_col
    slots = leaves // n_col
    groups = leaves // 4
    width_col = n_col * RANK
    turn_col = (lax.axis_index(COL) % 4).astype(jnp.int32).reshape(1)
    turn_row = (lax.axis_index(ROW) % 4).astype(jnp.int32).reshape(1)
    place = near_offsets.T + (jnp.arange(leaves, dtype=jnp.int32) + HALO)[None, :]
    near_rows = (
        near_blocks.reshape(leaves, 4, 32, LANES).transpose(0, 2, 1, 3).reshape(leaves, LANES, LANES)
    )
    z_shape = shape((n_col, RHS, slots * RANK), BF16)
    edge_shape = shape((RHS, HALO * LEAF), BF16)
    field = shape((RHS, count), F32)

    def halos(low, high):
        up = [(i, i + 1) for i in range(devices - 1)]
        down = [(b, a) for a, b in up]
        return lax.ppermute(high, ROW_COL, up), lax.ppermute(low, ROW_COL, down)

    def exchange(x, axes):
        return lax.all_to_all(x, axes, split_axis=0, concat_axis=0, tiled=True)

    def near(v, below, above):
        return call(
            near_kernel,
            [VMEM, VMEM, VMEM, SMEM, VMEM],
            field,
            [pltpu.VMEM((leaves // 2 + HALO, RHS, LANES), BF16)] * 2,
        )(v, below, above, place, near_wide)

    def first_mix(z):
        return call(
            first_mix_kernel, [VMEM, VMEM, SMEM], shape((n_row, RHS, width_col), BF16)
        )(z, mix_col.reshape(slots, width_col, width_col), turn_row)

    mix_second = mix_row.reshape(n_col, n_row * RANK, n_row * RANK)
    t2_scratch = [pltpu.VMEM((n_col, RHS, n_row * RANK), BF16)]

    v_wide, z, low, high = call(
        spread_v_kernel,
        [VMEM, VMEM, SMEM],
        (shape((groups, 4 * LEAF, 4 * RANK), BF16), z_shape, edge_shape, edge_shape),
        [pltpu.VMEM((8, 4 * LEAF, 4 * RANK), F32)],
    )(rhs, v_factor.reshape(leaves, 16, LANES), turn_col)
    z = exchange(z, COL)
    below, above = halos(low, high)
    step = 8
    near_wide = call(
        spread_near_kernel,
        [pl.BlockSpec((step, LANES, LANES), lambda i: (i, 0, 0))],
        shape((leaves // 2, LANES, 4 * LEAF), BF16),
        [pltpu.VMEM((step, LANES, LANES), F32), pltpu.VMEM((step, 2, LEAF, LANES), F32)],
        grid=(leaves // step,),
        out_specs=pl.BlockSpec((step // 2, LANES, 4 * LEAF), lambda i: (i, 0, 0)),
    )(near_rows)
    u_wide = call(
        spread_u_kernel,
        [VMEM],
        shape((groups, 4 * RANK, 4 * LEAF), BF16),
        [pltpu.VMEM((8, 2, 4 * RANK, LANES), F32)],
    )(u_factor.reshape(leaves, 16, LANES))
    t1 = exchange(first_mix(z), ROW)
    near_first = near(rhs, below, above)
    d, z, low, high = call(
        second_mix_kernel,
        [VMEM] * 5 + [SMEM],
        (field, z_shape, edge_shape, edge_shape),
        t2_scratch,
    )(t1, mix_second, u_wide, near_first, v_wide, turn_col)
    z = exchange(z, COL)
    below, above = halos(low, high)
    t1 = exchange(first_mix(z), ROW)
    near_second = near(d, below, above)
    e, sums = call(
        last_mix_kernel, [VMEM] * 6, (field, shape((devices, 8 * RHS), F32)), t2_scratch
    )(t1, mix_second, u_wide, near_second, rhs, d)
    sums = exchange(sums, ROW_COL)
    return call(finish_kernel, [VMEM] * 4, (field, field))(sums, rhs, d, e)


def solution(mesh):
    split = Mesh(mesh.devices.reshape(4, 2, 4, 4), ("row_0", "row_1", "col_0", "col_1"))
    return jax.shard_map(
        body,
        mesh=split,
        in_specs=(
            P(None, ROW_COL),
            P(ROW_COL, None, None),
            P(ROW_COL, None),
            P(ROW_COL, None),
            P(ROW, COL, None, None),
            P(ROW, COL, None, None),
            P(ROW_COL, None),
        ),
        out_specs=(P(None, ROW_COL), P(None, ROW_COL)),
        check_vma=False,
    )
```

```python
import jax
import jax.numpy as jnp
from jax import lax
from jax.experimental import pallas as pl
from jax.experimental.pallas import tpu as pltpu
from jax.sharding import Mesh
from jax.sharding import PartitionSpec as P

LEAF = 64
RANK = 32
HALO = 4
RHS = 32
LANES = 128
ROW_COL = ("row_0", "row_1", "col_0", "col_1")
ROW = ("row_0", "row_1")
COL = ("col_0", "col_1")
F32 = jnp.float32
BF16 = jnp.bfloat16


def dot(a, b):
    return jnp.dot(a, b, preferred_element_type=F32)


def dot_t(a, b):
    return lax.dot_general(a, b, (((1,), (1,)), ((), ())), preferred_element_type=F32)


def lane_group(rows):
    return lax.broadcasted_iota(jnp.int32, (rows, LANES), 1) // RANK


def lane_take(x, index):
    return jnp.take_along_axis(x, index, axis=1, mode="promise_in_bounds")


def lane_half(rows):
    return lax.broadcasted_iota(jnp.int32, (rows, LANES), 1) < LEAF


def pieces_of(source, target, sems, first, pieces, dim=0):
    size = source.shape[dim] // pieces
    at = [(slice(None),) * dim + (pl.ds(i * size, size),) for i in range(pieces)]
    return [pltpu.make_async_copy(source.at[x], target.at[x], sems.at[first + i]) for i, x in enumerate(at)]


class Queue:
    def __init__(self, copies, depth):
        self.copies, self.depth, self.done = copies, depth, 0
        for copy in copies[:depth]:
            copy.start()

    def wait(self, count=1):
        for _ in range(count):
            self.copies[self.done].wait()
            if self.done + self.depth < len(self.copies):
                self.copies[self.done + self.depth].start()
            self.done += 1


def wait_all(copies):
    for copy in copies:
        copy.wait()


def row_order(size, inner):
    row = lax.broadcasted_iota(jnp.int32, (size, size), 0)
    column = lax.broadcasted_iota(jnp.int32, (size, size), 1)
    outer = size // inner
    return jnp.where(column == row % outer * inner + row // outer, 1.0, 0.0).astype(BF16)


def leaf_rows(ref, sixteen, order):
    tiles = [ref[16 * sixteen : 16 * (sixteen + 1), t * LANES : (t + 1) * LANES] for t in range(16)]
    return dot(order, jnp.concatenate(tiles, axis=0))


def v_order():
    lane = lax.broadcasted_iota(jnp.int32, (RHS, LANES), 1)
    return lane // LEAF * LEAF + lane % 16 * 4 + lane % LEAF // 16


def compress(x, narrow, order, masks):
    lhs = jnp.concatenate([lane_take(x[:, t * LANES : (t + 1) * LANES], order).astype(BF16) for t in range(2)], axis=1)
    return dot(lhs, jnp.concatenate([narrow * mask for mask in masks], axis=0))


def group_masks(rows):
    group = lane_group(rows)
    return [jnp.where(group == leaf, 1.0, 0.0).astype(BF16) for leaf in range(4)]


def put_edges(v_ref, z_ref, place_ref):
    n_col, _, width = z_ref.shape
    edge = HALO * LEAF
    z_ref[lax.rem(place_ref[0] + 1, n_col), :, width - edge :] = v_ref[:, v_ref.shape[1] - edge :].astype(BF16)
    z_ref[lax.rem(place_ref[0] + n_col - 1, n_col), :, width - edge :] = v_ref[:, :edge].astype(BF16)


def spread_v_kernel(rhs_hbm, v_hbm, mix_hbm, turn_ref, vc_ref, z_ref, rhs_ref, mix_ref, v_ref, sems):
    mix_in = pieces_of(mix_hbm, mix_ref, sems, 8, 8)
    queue = Queue(pieces_of(v_hbm, v_ref, sems, 0, 4) + pieces_of(rhs_hbm, rhs_ref, sems, 4, 4, 1), 8)
    for copy in mix_in:
        copy.start()
    group = lane_group(16)
    shift = turn_ref[0] % 4 * RANK
    order = row_order(256, 16)
    groups = vc_ref.shape[0]
    for sixteen in range(groups // 4):
        if sixteen % (groups // 16) == 0:
            queue.wait()
        rows = leaf_rows(v_ref, sixteen, order)
        for h in range(4):
            of_leaf = [rows[16 * leaf : 16 * (leaf + 1)] for leaf in range(4 * h, 4 * h + 4)]
            for ur in range(4):
                x = of_leaf[ur]
                for leaf in range(4):
                    if leaf != ur:
                        x = jnp.where(group == leaf, pltpu.roll(of_leaf[leaf], (leaf - ur) * RANK % LANES, 1), x)
                vc_ref[4 * sixteen + h, 16 * ur : 16 * (ur + 1), :] = x.astype(BF16)
    masks = group_masks(LEAF)
    lanes = v_order()
    for g in range(groups):
        if g % (groups // 4) == 0:
            queue.wait()
        part = compress(rhs_ref[:, 256 * g : 256 * (g + 1)], vc_ref[g], lanes, masks)
        z_ref[g // 2, :, (g % 2) * LANES : (g % 2 + 1) * LANES] = pltpu.roll(part, shift, 1).astype(BF16)
    put_edges(rhs_ref, z_ref, turn_ref)
    wait_all(mix_in)


def spread_u(u_ref, uc_ref):
    half = lane_half(16)
    order = row_order(256, 16)
    for sixteen in range(uc_ref.shape[0] // 4):
        rows = leaf_rows(u_ref, sixteen, order)
        for h in range(4):
            for tile in range(2):
                leaf = 4 * h + 2 * tile
                a, b = rows[16 * leaf : 16 * (leaf + 1)], rows[16 * (leaf + 1) : 16 * (leaf + 2)]
                lanes = slice(tile * LANES, (tile + 1) * LANES)
                uc_ref[4 * sixteen + h, :16, lanes] = jnp.where(half, a, pltpu.roll(b, LEAF, 1)).astype(BF16)
                uc_ref[4 * sixteen + h, 16:, lanes] = jnp.where(half, pltpu.roll(a, LEAF, 1), b).astype(BF16)


def spread_near(near_ref, out_ref):
    half = lane_half(32)
    order = row_order(LANES, 4)
    for pair in range(out_ref.shape[0]):
        both = dot(order, jnp.concatenate([near_ref[2 * pair], near_ref[2 * pair + 1]], axis=1))
        for leaf in range(2):
            block = [both[32 * b : 32 * (b + 1), leaf * LANES : (leaf + 1) * LANES] for b in range(4)]
            for h in range(2):
                first, second = block[2 * h], block[2 * h + 1]
                even = jnp.where(half, first, pltpu.roll(second, LEAF, 1))
                odd = jnp.where(half, pltpu.roll(first, LEAF, 1), second)
                lanes = slice(h * LANES, (h + 1) * LANES)
                out_ref[pair, leaf * LEAF : leaf * LEAF + 32, lanes] = even.astype(BF16)
                out_ref[pair, leaf * LEAF + 32 : leaf * LEAF + 64, lanes] = odd.astype(BF16)


def near_kernel(v_ref, z_ref, t1_ref, turn_ref, place_ref, near_ref, out_ref, left, right):
    half = lane_half(RHS)
    lane = lax.broadcasted_iota(jnp.int32, (RHS, LANES), 1)
    order = lane // LEAF * LEAF + lane % 2 * 32 + lane % LEAF // 2
    edge = HALO // 2
    tiles = v_ref.shape[1] // LANES

    def put(t, x):
        turned = pltpu.roll(x, LEAF, 1)
        left[2 * t] = jnp.where(half, x, 0.0).astype(BF16)
        left[2 * t + 1] = jnp.where(half, turned, 0.0).astype(BF16)
        right[2 * t] = jnp.where(half, 0.0, turned).astype(BF16)
        right[2 * t + 1] = jnp.where(half, 0.0, x).astype(BF16)

    column, row = turn_ref[0], turn_ref[1]
    n_col, n_row = z_ref.shape[0], t1_ref.shape[0]
    z_lanes = slice(z_ref.shape[2] - HALO * LEAF, z_ref.shape[2])
    t1_lanes = slice(t1_ref.shape[2] - HALO * LEAF, t1_ref.shape[2])

    def beside(step, at_end, outside):
        near_by = z_ref[lax.clamp(0, column + step, n_col - 1), :, z_lanes].astype(F32)
        next_row = t1_ref[lax.clamp(0, row + step, n_row - 1), :, t1_lanes].astype(F32)
        return jnp.where(at_end, jnp.where(outside, 0.0, next_row), near_by)

    below = beside(-1, column == 0, row == 0)
    above = beside(1, column == n_col - 1, row == n_row - 1)
    for t in range(edge):
        put(t, below[:, t * LANES : (t + 1) * LANES])
        put(edge + tiles + t, above[:, t * LANES : (t + 1) * LANES])
    for t in range(tiles):
        put(edge + t, v_ref[:, t * LANES : (t + 1) * LANES])
    for pair in range(tiles):
        lhs = [
            jnp.concatenate(
                [left[place_ref[2 * h, leaf] + (leaf + HALO)] + right[place_ref[2 * h + 1, leaf] + (leaf + HALO)] for h in range(2)], axis=1
            )
            for leaf in (2 * pair, 2 * pair + 1)
        ]
        both = dot_t(jnp.concatenate(lhs, axis=0), near_ref[pair])
        out_ref[:, pair * LANES : (pair + 1) * LANES] = lane_take(jnp.where(half, both[:RHS], both[RHS:]), order)


def first_near_kernel(rows_ref, u_ref, v_ref, z_ref, t1_ref, turn_ref, place_ref, wide_ref, uc_ref, out_ref, left, right):
    spread_near(rows_ref, wide_ref)
    spread_u(u_ref, uc_ref)
    near_kernel(v_ref, z_ref, t1_ref, turn_ref, place_ref, wide_ref, out_ref, left, right)


def gather_lanes(parts, where_from, group):
    x = parts[(0 - where_from) % 4]
    for q in range(1, 4):
        x = jnp.where(group == q, parts[(q - where_from) % 4], x)
    return x


def turned_rows(ref_rows, count, where_from):
    order = [4 * four + (q - where_from) % 4 for four in range(count // 4) for q in range(4)]
    return jnp.concatenate([ref_rows[c * RANK : (c + 1) * RANK] for c in order], axis=0)


def first_mix_kernel(z_ref, mix_ref, turn_ref, out_ref):
    slots = mix_ref.shape[0]
    n_col = z_ref.shape[0]
    group = lane_group(RHS)
    shift = turn_ref[1] % 4 * RANK
    for j in range(slots):
        tile = j // 4
        lhs = jnp.concatenate(
            [
                gather_lanes(
                    [z_ref[4 * four + c, :, tile * LANES : (tile + 1) * LANES] for c in range(4)], j % 4, group
                )
                for four in range(n_col // 4)
            ],
            axis=1,
        )
        out = dot(lhs, turned_rows(mix_ref[j], n_col, j % 4))
        for t in range(out.shape[1] // LANES):
            out_ref[j, :, t * LANES : (t + 1) * LANES] = pltpu.roll(
                out[:, t * LANES : (t + 1) * LANES], shift, 1
            ).astype(BF16)
    first = turn_ref[0] == 0
    other_end = jnp.where(first, n_col - 1, 0)
    beside = lax.clamp(0, turn_ref[1] + jnp.where(first, 1, -1), slots - 1)
    edge = HALO * LEAF
    out_ref[beside, :, out_ref.shape[2] - edge :] = z_ref[other_end, :, z_ref.shape[2] - edge :]


def second_mix(t1_ref, mix_ref, t2_ref):
    n_row = t1_ref.shape[0]
    group = lane_group(RHS)
    count = mix_ref.shape[0]
    lane = lax.broadcasted_iota(jnp.int32, (RHS, LANES), 1)
    order = lane // RANK * RANK + lane % 16 * 2 + lane % RANK // 16
    for p in range(count):
        tile = p // 4
        lhs = jnp.concatenate(
            [
                gather_lanes(
                    [t1_ref[4 * four + r, :, tile * LANES : (tile + 1) * LANES] for r in range(4)], p % 4, group
                )
                for four in range(n_row // 4)
            ],
            axis=1,
        )
        out = dot(lhs, turned_rows(mix_ref[p], n_row, p % 4))
        for t in range(2):
            lanes = slice(t * LANES, (t + 1) * LANES)
            t2_ref[p, :, lanes] = lane_take(out[:, lanes], order).astype(BF16)


def expand_masks():
    lane = lax.broadcasted_iota(jnp.int32, (RANK, 2 * LANES), 1)
    return [jnp.where(lane // LEAF == leaf, 1.0, 0.0).astype(BF16) for leaf in range(4)]


def far_tile(t2_ref, uc_ref, masks, g):
    narrow = uc_ref[g]
    wide = jnp.concatenate([narrow * mask for mask in masks], axis=0)
    return dot(t2_ref[g // 2, :, (g % 2) * LANES : (g % 2 + 1) * LANES], wide)


def second_mix_kernel(
    t1_ref, mix_ref, uc_ref, near_ref, vc_ref, turn_ref, d_ref, z_ref, t2_ref
):
    second_mix(t1_ref, mix_ref, t2_ref)
    shift = turn_ref[0] % 4 * RANK
    groups = uc_ref.shape[0]
    masks = expand_masks()
    for g in range(groups):
        lanes = slice(256 * g, 256 * (g + 1))
        d_ref[:, lanes] = far_tile(t2_ref, uc_ref, masks, g) + near_ref[:, lanes]
    masks = group_masks(LEAF)
    order = v_order()
    for g in range(groups):
        part = compress(d_ref[:, 256 * g : 256 * (g + 1)], vc_ref[g], order, masks)
        z_ref[g // 2, :, (g % 2) * LANES : (g % 2 + 1) * LANES] = pltpu.roll(part, shift, 1).astype(BF16)
    put_edges(d_ref, z_ref, turn_ref)


def last_mix_kernel(t1_ref, mix_ref, uc_ref, near_ref, rhs_ref, d_ref, e_ref, sums_ref, t2_ref):
    second_mix(t1_ref, mix_ref, t2_ref)
    masks = expand_masks()
    total = [jnp.zeros((RHS, LANES), F32) for _ in range(6)]
    for g in range(uc_ref.shape[0]):
        wide = far_tile(t2_ref, uc_ref, masks, g) + near_ref[:, 256 * g : 256 * (g + 1)]
        e_ref[:, 256 * g : 256 * (g + 1)] = wide
        for t in range(2):
            lanes = slice(256 * g + LANES * t, 256 * g + LANES * (t + 1))
            r, d, e = rhs_ref[:, lanes], d_ref[:, lanes], wide[:, LANES * t : LANES * (t + 1)]
            terms = (r * r, r * d, d * d, r * e, d * e, e * e)
            total = [a + b for a, b in zip(total, terms)]
    stacked = jnp.concatenate(total + [jnp.zeros((2 * RHS, LANES), F32)], axis=0)
    row = jnp.sum(stacked.T, axis=0, keepdims=True)
    sums_ref[...] = jnp.broadcast_to(row[None], sums_ref.shape)


def finish_kernel(sums_ref, rhs_ref, d_ref, e_ref, solution_hbm, residual_hbm, solution_ref, residual_ref, sems):
    row = jnp.sum(sums_ref[...], axis=0)
    columns = jnp.broadcast_to(row, (LANES, row.shape[1])).T
    rr, rd, dd, re, de, ee = [columns[i * RHS : (i + 1) * RHS] for i in range(6)]
    scale = 1.0 / rr
    alpha = rd * scale
    h21_sq = (dd - alpha * rd) * scale
    h11 = 1.0 + alpha
    cross = re * scale - alpha * alpha
    inverse = 1.0 / h21_sq
    gain = ((de - alpha * dd - alpha * re + alpha * (alpha * rd)) * scale) * inverse
    h22 = 1.0 + gain
    spread = ((ee - 2.0 * alpha * de + alpha * (alpha * dd)) * scale) * inverse
    h32_sq = spread - gain * gain - cross * (cross * inverse)
    minor = h11 * h22 - cross
    determ = minor * minor + h32_sq * (h11 * h11 + h21_sq)
    x_first = (h22 * minor + h11 * h32_sq) / determ
    x_second = -minor / determ
    on_rhs = x_first - alpha * x_second
    on_d = x_first + x_second * (1.0 - alpha)
    solution_out = pieces_of(solution_ref, solution_hbm, sems, 0, 4, 1)
    residual_out = pieces_of(residual_ref, residual_hbm, sems, 4, 4, 1)
    tiles = rhs_ref.shape[1] // LANES
    for t in range(tiles):
        lanes = slice(t * LANES, (t + 1) * LANES)
        r, d, e = rhs_ref[:, lanes], d_ref[:, lanes], e_ref[:, lanes]
        solution_ref[:, lanes] = on_rhs * r + x_second * d
        residual_ref[:, lanes] = (1.0 - on_rhs) * r - on_d * d - x_second * e
        if (t + 1) % (tiles // 4) == 0:
            solution_out[t // (tiles // 4)].start()
            residual_out[t // (tiles // 4)].start()
    wait_all(solution_out + residual_out)


VMEM = pl.BlockSpec(memory_space=pltpu.VMEM)
HBM = pl.BlockSpec(memory_space=pltpu.HBM)
SMEM = pl.BlockSpec(memory_space=pltpu.SMEM)
MIB = 1 << 20
KEPT = pltpu.VMEM
FAR_OFF = pltpu.HBM


def call(kernel, in_specs, outs, scratch=(), sems=0, limit=8):
    run = pl.pallas_call(
        kernel,
        in_specs=in_specs,
        out_shape=[space(dims, dtype) for space, dims, dtype, _ in outs],
        out_specs=[spec for *_, spec in outs],
        scratch_shapes=[pltpu.VMEM(*x) for x in scratch] + [pltpu.SemaphoreType.DMA((sems,))] * (sems > 0),
        cost_estimate=pl.CostEstimate(flops=1_000_000, bytes_accessed=1_000_000, transcendentals=0),
        compiler_params=pltpu.CompilerParams(vmem_limit_bytes=limit * MIB),
        name=kernel.__name__,
    )

    def placed(*args):
        spaces = {id(VMEM): pltpu.VMEM, id(HBM): pltpu.HBM}
        args = [
            pltpu.with_memory_space_constraint(x, spaces[id(spec)]) if id(spec) in spaces else x
            for x, spec in zip(args, in_specs)
        ]
        out = run(*args)
        return out if len(outs) > 1 else out[0]

    return placed


def body(rhs, near_blocks, near_offsets, v_factor, mix_col, mix_row, u_factor):
    count = rhs.shape[1]
    leaves = near_offsets.shape[0]
    n_row = lax.axis_size(ROW)
    n_col = lax.axis_size(COL)
    devices = n_row * n_col
    slots = leaves // n_col
    groups = leaves // 4
    width_col = n_col * RANK
    width_row = n_row * RANK
    turn = jnp.stack([lax.axis_index(COL), lax.axis_index(ROW)]).astype(jnp.int32)
    place = near_offsets.T
    near_rows = (
        near_blocks.reshape(leaves, 4, 32, LANES).transpose(0, 2, 1, 3).reshape(leaves, LANES, LANES)
    )
    mix_first = mix_col.reshape(slots, width_col, width_col)
    mix_second = mix_row.reshape(n_col, width_row, width_row)
    field = ((RHS, count), F32)
    vc_shape = ((groups, LEAF, LANES), BF16)
    uc_shape = ((groups, RANK, 2 * LANES), BF16)
    wide_shape = ((leaves // 2, LANES, 4 * LEAF), BF16)
    z_out = (KEPT, (n_col, RHS, slots * RANK + HALO * LEAF), BF16, VMEM)
    t1_out = (KEPT, (n_row, RHS, width_col + HALO * LEAF), BF16, VMEM)
    t2_shape = ((n_col, RHS, width_row), BF16)

    def exchange(x, axes):
        return lax.all_to_all(x, axes, split_axis=0, concat_axis=0, tiled=True)

    store = ((leaves + 2 * HALO, RHS, LANES), BF16)

    vc, z, rhs_kept, mix_kept = call(
        spread_v_kernel,
        [HBM, HBM, HBM, SMEM],
        [(KEPT, *vc_shape, VMEM), z_out, (KEPT, *field, VMEM), (KEPT, mix_first.shape, BF16, VMEM)],
        [(v_factor.shape, BF16)],
        16,
    )(rhs, v_factor, mix_first, turn)

    def first_mix(z):
        return call(first_mix_kernel, [VMEM, VMEM, SMEM], [t1_out])(z, mix_kept, turn)

    z = exchange(z, COL)
    t1 = exchange(first_mix(z), ROW)
    t1, place = lax.optimization_barrier((t1, place))
    near_wide, uc, near_first = call(
        first_near_kernel,
        [VMEM, VMEM, VMEM, VMEM, VMEM, SMEM, SMEM],
        [(KEPT, *wide_shape, VMEM), (KEPT, *uc_shape, VMEM), (KEPT, *field, VMEM)],
        [store, store],
    )(near_rows, u_factor, rhs_kept, z, t1, turn, place)
    d, z = call(
        second_mix_kernel, [VMEM] * 5 + [SMEM], [(KEPT, *field, VMEM), z_out], [t2_shape]
    )(t1, mix_second, uc, near_first, vc, turn)
    z = exchange(z, COL)
    t1 = exchange(first_mix(z), ROW)
    near_second = call(
        near_kernel, [VMEM, VMEM, VMEM, SMEM, SMEM, VMEM], [(KEPT, *field, VMEM)], [store, store]
    )(d, z, t1, turn, place, near_wide)
    e, sums = call(
        last_mix_kernel,
        [VMEM] * 6,
        [(KEPT, *field, VMEM), (KEPT, (devices, 1, 8 * RHS), F32, VMEM)],
        [t2_shape],
    )(t1, mix_second, uc, near_second, rhs_kept, d)
    sums = exchange(sums, ROW_COL)
    return tuple(
        call(
            finish_kernel, [VMEM] * 4, [(FAR_OFF, *field, HBM)] * 2, [field, field], 8
        )(sums, rhs_kept, d, e)
    )


def solution(mesh):
    split = Mesh(mesh.devices.reshape(4, 2, 4, 4), ("row_0", "row_1", "col_0", "col_1"))
    return jax.shard_map(
        body,
        mesh=split,
        in_specs=(
            P(None, ROW_COL),
            P(ROW_COL, None, None),
            P(ROW_COL, None),
            P(ROW_COL, None),
            P(ROW, COL, None, None),
            P(ROW, COL, None, None),
            P(ROW_COL, None),
        ),
        out_specs=(P(None, ROW_COL), P(None, ROW_COL)),
        check_vma=False,
    )
```

```python
import jax
import jax.numpy as jnp
from jax import lax
from jax.experimental import pallas as pl
from jax.experimental.pallas import tpu as pltpu
from jax.sharding import Mesh
from jax.sharding import PartitionSpec as P

LEAF = 64
RANK = 32
HALO = 4
RHS = 32
LANES = 128
ROW_COL = ("row_0", "row_1", "col_0", "col_1")
ROW = ("row_0", "row_1")
COL = ("col_0", "col_1")
F32 = jnp.float32
BF16 = jnp.bfloat16


def dot(a, b):
    return jnp.dot(a, b, preferred_element_type=F32)


def dot_t(a, b):
    return lax.dot_general(a, b, (((1,), (1,)), ((), ())), preferred_element_type=F32)


def lane_group(rows):
    return lax.broadcasted_iota(jnp.int32, (rows, LANES), 1) // RANK


def lane_take(x, index):
    return jnp.take_along_axis(x, index, axis=1, mode="promise_in_bounds")


def lane_half(rows):
    return lax.broadcasted_iota(jnp.int32, (rows, LANES), 1) < LEAF


def column_index():
    return lax.axis_index("col_0") * lax.axis_size("col_1") + lax.axis_index("col_1")


def row_index():
    return lax.axis_index("row_0") * lax.axis_size("row_1") + lax.axis_index("row_1")


def pieces_of(source, target, sems, first, pieces, dim=0):
    size = source.shape[dim] // pieces
    at = [(slice(None),) * dim + (pl.ds(i * size, size),) for i in range(pieces)]
    return [pltpu.make_async_copy(source.at[x], target.at[x], sems.at[first + i]) for i, x in enumerate(at)]


class Queue:
    def __init__(self, copies, depth):
        self.copies, self.depth, self.done = copies, depth, 0
        for copy in copies[:depth]:
            copy.start()

    def wait(self, count=1):
        for _ in range(count):
            self.copies[self.done].wait()
            if self.done + self.depth < len(self.copies):
                self.copies[self.done + self.depth].start()
            self.done += 1


def wait_all(copies):
    for copy in copies:
        copy.wait()


def row_order(size, inner):
    row = lax.broadcasted_iota(jnp.int32, (size, size), 0)
    column = lax.broadcasted_iota(jnp.int32, (size, size), 1)
    outer = size // inner
    return jnp.where(column == row % outer * inner + row // outer, 1.0, 0.0).astype(BF16)


def leaf_rows(ref, sixteen, order):
    tiles = [ref[16 * sixteen : 16 * (sixteen + 1), t * LANES : (t + 1) * LANES] for t in range(16)]
    return dot(order, jnp.concatenate(tiles, axis=0))


def v_order():
    lane = lax.broadcasted_iota(jnp.int32, (RHS, LANES), 1)
    return lane // LEAF * LEAF + lane % 16 * 4 + lane % LEAF // 16


def compress(x, narrow, order, masks):
    lhs = jnp.concatenate([lane_take(x[:, t * LANES : (t + 1) * LANES], order).astype(BF16) for t in range(2)], axis=1)
    return dot(lhs, jnp.concatenate([narrow * mask for mask in masks], axis=0))


def group_masks(rows):
    group = lane_group(rows)
    return [jnp.where(group == leaf, 1.0, 0.0).astype(BF16) for leaf in range(4)]


def put_edges(v_ref, z_ref):
    n_col, _, width = z_ref.shape
    edge = HALO * LEAF
    z_ref[lax.rem(column_index() + 1, n_col), :, width - edge :] = v_ref[:, v_ref.shape[1] - edge :].astype(BF16)
    z_ref[lax.rem(column_index() + n_col - 1, n_col), :, width - edge :] = v_ref[:, :edge].astype(BF16)


def spread_v_kernel(rhs_hbm, v_hbm, mix_hbm, vc_ref, z_ref, rhs_ref, mix_ref, v_ref, sems):
    queue = Queue(pieces_of(v_hbm, v_ref, sems, 0, 4) + pieces_of(rhs_hbm, rhs_ref, sems, 4, 4, 1), 8)
    mix_in = pieces_of(mix_hbm, mix_ref, sems, 8, 8)
    for copy in mix_in:
        copy.start()
    group = lane_group(16)
    shift = column_index() % 4 * RANK
    order = row_order(256, 16)
    groups = vc_ref.shape[0]
    for sixteen in range(groups // 4):
        if sixteen % (groups // 16) == 0:
            queue.wait()
        rows = leaf_rows(v_ref, sixteen, order)
        for h in range(4):
            of_leaf = [rows[16 * leaf : 16 * (leaf + 1)] for leaf in range(4 * h, 4 * h + 4)]
            for ur in range(4):
                x = of_leaf[ur]
                for leaf in range(4):
                    if leaf != ur:
                        x = jnp.where(group == leaf, pltpu.roll(of_leaf[leaf], (leaf - ur) * RANK % LANES, 1), x)
                vc_ref[4 * sixteen + h, 16 * ur : 16 * (ur + 1), :] = x.astype(BF16)
    masks = group_masks(LEAF)
    lanes = v_order()
    for g in range(groups):
        if g % (groups // 4) == 0:
            queue.wait()
        part = compress(rhs_ref[:, 256 * g : 256 * (g + 1)], vc_ref[g], lanes, masks)
        z_ref[g // 2, :, (g % 2) * LANES : (g % 2 + 1) * LANES] = pltpu.roll(part, shift, 1).astype(BF16)
    put_edges(rhs_ref, z_ref)
    wait_all(mix_in)


def spread_u(u_ref, uc_ref):
    half = lane_half(16)
    order = row_order(256, 16)
    for sixteen in range(uc_ref.shape[0] // 4):
        rows = leaf_rows(u_ref, sixteen, order)
        for h in range(4):
            for tile in range(2):
                leaf = 4 * h + 2 * tile
                a, b = rows[16 * leaf : 16 * (leaf + 1)], rows[16 * (leaf + 1) : 16 * (leaf + 2)]
                lanes = slice(tile * LANES, (tile + 1) * LANES)
                uc_ref[4 * sixteen + h, :16, lanes] = jnp.where(half, a, pltpu.roll(b, LEAF, 1)).astype(BF16)
                uc_ref[4 * sixteen + h, 16:, lanes] = jnp.where(half, pltpu.roll(a, LEAF, 1), b).astype(BF16)


def spread_near(near_ref, out_ref):
    half = lane_half(32)
    order = row_order(LANES, 4)
    for pair in range(out_ref.shape[0]):
        both = dot(order, jnp.concatenate([near_ref[2 * pair], near_ref[2 * pair + 1]], axis=1))
        for leaf in range(2):
            block = [both[32 * b : 32 * (b + 1), leaf * LANES : (leaf + 1) * LANES] for b in range(4)]
            for h in range(2):
                first, second = block[2 * h], block[2 * h + 1]
                even = jnp.where(half, first, pltpu.roll(second, LEAF, 1))
                odd = jnp.where(half, pltpu.roll(first, LEAF, 1), second)
                lanes = slice(h * LANES, (h + 1) * LANES)
                out_ref[pair, leaf * LEAF : leaf * LEAF + 32, lanes] = even.astype(BF16)
                out_ref[pair, leaf * LEAF + 32 : leaf * LEAF + 64, lanes] = odd.astype(BF16)


def near_product(v_ref, z_ref, t1_ref, place_ref, near_ref, out_ref, left, right, table):
    half = lane_half(RHS)
    lane = lax.broadcasted_iota(jnp.int32, (RHS, LANES), 1)
    order = lane // LEAF * LEAF + lane % 2 * 32 + lane % LEAF // 2
    edge = HALO // 2
    tiles = v_ref.shape[1] // LANES

    def put(t, x):
        turned = pltpu.roll(x, LEAF, 1)
        left[2 * t] = jnp.where(half, x, 0.0).astype(BF16)
        left[2 * t + 1] = jnp.where(half, turned, 0.0).astype(BF16)
        right[2 * t] = jnp.where(half, 0.0, turned).astype(BF16)
        right[2 * t + 1] = jnp.where(half, 0.0, x).astype(BF16)

    column, row = column_index(), row_index()
    n_col, n_row = z_ref.shape[0], t1_ref.shape[0]
    z_lanes = slice(z_ref.shape[2] - HALO * LEAF, z_ref.shape[2])
    t1_lanes = slice(t1_ref.shape[2] - HALO * LEAF, t1_ref.shape[2])

    def beside(step, at_end, outside):
        near_by = z_ref[lax.clamp(0, column + step, n_col - 1), :, z_lanes].astype(F32)
        next_row = t1_ref[lax.clamp(0, row + step, n_row - 1), :, t1_lanes].astype(F32)
        return jnp.where(at_end, jnp.where(outside, 0.0, next_row), near_by)

    below = beside(-1, column == 0, row == 0)
    above = beside(1, column == n_col - 1, row == n_row - 1)
    for t in range(edge):
        put(t, below[:, t * LANES : (t + 1) * LANES])
        put(edge + tiles + t, above[:, t * LANES : (t + 1) * LANES])
    for t in range(tiles):
        put(edge + t, v_ref[:, t * LANES : (t + 1) * LANES])
    table.wait()
    for pair in range(tiles):
        lhs = [
            jnp.concatenate(
                [left[place_ref[2 * h, leaf] + (leaf + HALO)] + right[place_ref[2 * h + 1, leaf] + (leaf + HALO)] for h in range(2)], axis=1
            )
            for leaf in (2 * pair, 2 * pair + 1)
        ]
        both = dot_t(jnp.concatenate(lhs, axis=0), near_ref[pair])
        out_ref[:, pair * LANES : (pair + 1) * LANES] = lane_take(jnp.where(half, both[:RHS], both[RHS:]), order)


def gather_lanes(parts, where_from, group):
    x = parts[(0 - where_from) % 4]
    for q in range(1, 4):
        x = jnp.where(group == q, parts[(q - where_from) % 4], x)
    return x


def turned_rows(ref_rows, count, where_from):
    order = [4 * four + (q - where_from) % 4 for four in range(count // 4) for q in range(4)]
    return jnp.concatenate([ref_rows[c * RANK : (c + 1) * RANK] for c in order], axis=0)


def first_mix_kernel(z_ref, mix_ref, out_ref):
    slots = mix_ref.shape[0]
    n_col = z_ref.shape[0]
    group = lane_group(RHS)
    shift = row_index() % 4 * RANK
    for j in range(slots):
        tile = j // 4
        lhs = jnp.concatenate(
            [
                gather_lanes(
                    [z_ref[4 * four + c, :, tile * LANES : (tile + 1) * LANES] for c in range(4)], j % 4, group
                )
                for four in range(n_col // 4)
            ],
            axis=1,
        )
        out = dot(lhs, turned_rows(mix_ref[j], n_col, j % 4))
        for t in range(out.shape[1] // LANES):
            out_ref[j, :, t * LANES : (t + 1) * LANES] = pltpu.roll(
                out[:, t * LANES : (t + 1) * LANES], shift, 1
            ).astype(BF16)
    first = column_index() == 0
    other_end = jnp.where(first, n_col - 1, 0)
    beside = lax.clamp(0, row_index() + jnp.where(first, 1, -1), slots - 1)
    edge = HALO * LEAF
    out_ref[beside, :, out_ref.shape[2] - edge :] = z_ref[other_end, :, z_ref.shape[2] - edge :]


def second_mix(t1_ref, mix_ref, t2_ref):
    n_row = t1_ref.shape[0]
    group = lane_group(RHS)
    count = mix_ref.shape[0]
    lane = lax.broadcasted_iota(jnp.int32, (RHS, LANES), 1)
    order = lane // RANK * RANK + lane % 16 * 2 + lane % RANK // 16
    for p in range(count):
        tile = p // 4
        lhs = jnp.concatenate(
            [
                gather_lanes(
                    [t1_ref[4 * four + r, :, tile * LANES : (tile + 1) * LANES] for r in range(4)], p % 4, group
                )
                for four in range(n_row // 4)
            ],
            axis=1,
        )
        out = dot(lhs, turned_rows(mix_ref[p], n_row, p % 4))
        for t in range(2):
            lanes = slice(t * LANES, (t + 1) * LANES)
            t2_ref[p, :, lanes] = lane_take(out[:, lanes], order).astype(BF16)


def expand_masks():
    lane = lax.broadcasted_iota(jnp.int32, (RANK, 2 * LANES), 1)
    return [jnp.where(lane // LEAF == leaf, 1.0, 0.0).astype(BF16) for leaf in range(4)]


def far_tile(t2_ref, uc_ref, masks, g):
    narrow = uc_ref[g]
    wide = jnp.concatenate([narrow * mask for mask in masks], axis=0)
    return dot(t2_ref[g // 2, :, (g % 2) * LANES : (g % 2 + 1) * LANES], wide)


def first_apply_kernel(
    rows_ref, u_ref, v_ref, in_ref, t1_ref, place_hbm, mix_ref, vc_ref,
    wide_ref, uc_ref, d_ref, z_ref,
    near_ref, left, right, t2_ref, place_ref, sem,
):
    table = pltpu.make_async_copy(place_hbm, place_ref, sem)
    table.start()
    spread_near(rows_ref, wide_ref)
    spread_u(u_ref, uc_ref)
    second_mix(t1_ref, mix_ref, t2_ref)
    near_product(v_ref, in_ref, t1_ref, place_ref, wide_ref, near_ref, left, right, table)
    shift = column_index() % 4 * RANK
    groups = uc_ref.shape[0]
    masks = expand_masks()
    for g in range(groups):
        lanes = slice(256 * g, 256 * (g + 1))
        d_ref[:, lanes] = far_tile(t2_ref, uc_ref, masks, g) + near_ref[:, lanes]
    masks = group_masks(LEAF)
    order = v_order()
    for g in range(groups):
        part = compress(d_ref[:, 256 * g : 256 * (g + 1)], vc_ref[g], order, masks)
        z_ref[g // 2, :, (g % 2) * LANES : (g % 2 + 1) * LANES] = pltpu.roll(part, shift, 1).astype(BF16)
    put_edges(d_ref, z_ref)


def second_apply_kernel(
    t1_ref, mix_ref, uc_ref, wide_ref, in_ref, place_hbm, rhs_ref, d_ref,
    e_ref, sums_ref,
    near_ref, left, right, t2_ref, place_ref, sem,
):
    table = pltpu.make_async_copy(place_hbm, place_ref, sem)
    table.start()
    second_mix(t1_ref, mix_ref, t2_ref)
    near_product(d_ref, in_ref, t1_ref, place_ref, wide_ref, near_ref, left, right, table)
    masks = expand_masks()
    total = [jnp.zeros((RHS, LANES), F32) for _ in range(6)]
    for g in range(uc_ref.shape[0]):
        wide = far_tile(t2_ref, uc_ref, masks, g) + near_ref[:, 256 * g : 256 * (g + 1)]
        e_ref[:, 256 * g : 256 * (g + 1)] = wide
        for t in range(2):
            lanes = slice(256 * g + LANES * t, 256 * g + LANES * (t + 1))
            r, d, e = rhs_ref[:, lanes], d_ref[:, lanes], wide[:, LANES * t : LANES * (t + 1)]
            terms = (r * r, r * d, d * d, r * e, d * e, e * e)
            total = [a + b for a, b in zip(total, terms)]
    stacked = jnp.concatenate(total + [jnp.zeros((2 * RHS, LANES), F32)], axis=0)
    row = jnp.sum(stacked.T, axis=0, keepdims=True)
    sums_ref[...] = jnp.broadcast_to(row[None], sums_ref.shape)


def finish_kernel(sums_ref, rhs_ref, d_ref, e_ref, solution_hbm, residual_hbm, solution_ref, residual_ref, sems):
    row = jnp.sum(sums_ref[...], axis=0)
    columns = jnp.broadcast_to(row, (LANES, row.shape[1])).T
    rr, rd, dd, re, de, ee = [columns[i * RHS : (i + 1) * RHS] for i in range(6)]
    scale = 1.0 / rr
    alpha = rd * scale
    h21_sq = (dd - alpha * rd) * scale
    h11 = 1.0 + alpha
    cross = re * scale - alpha * alpha
    inverse = 1.0 / h21_sq
    gain = ((de - alpha * dd - alpha * re + alpha * (alpha * rd)) * scale) * inverse
    h22 = 1.0 + gain
    spread = ((ee - 2.0 * alpha * de + alpha * (alpha * dd)) * scale) * inverse
    h32_sq = spread - gain * gain - cross * (cross * inverse)
    minor = h11 * h22 - cross
    determ = minor * minor + h32_sq * (h11 * h11 + h21_sq)
    x_first = (h22 * minor + h11 * h32_sq) / determ
    x_second = -minor / determ
    on_rhs = x_first - alpha * x_second
    on_d = x_first + x_second * (1.0 - alpha)
    solution_out = pieces_of(solution_ref, solution_hbm, sems, 0, 4, 1)
    residual_out = pieces_of(residual_ref, residual_hbm, sems, 4, 4, 1)
    tiles = rhs_ref.shape[1] // LANES
    for t in range(tiles):
        lanes = slice(t * LANES, (t + 1) * LANES)
        r, d, e = rhs_ref[:, lanes], d_ref[:, lanes], e_ref[:, lanes]
        solution_ref[:, lanes] = on_rhs * r + x_second * d
        residual_ref[:, lanes] = (1.0 - on_rhs) * r - on_d * d - x_second * e
        if (t + 1) % (tiles // 4) == 0:
            solution_out[t // (tiles // 4)].start()
            residual_out[t // (tiles // 4)].start()
    wait_all(solution_out + residual_out)


VMEM = pl.BlockSpec(memory_space=pltpu.VMEM)
HBM = pl.BlockSpec(memory_space=pltpu.HBM)
SMEM = pl.BlockSpec(memory_space=pltpu.SMEM)
MIB = 1 << 20
KEPT = pltpu.VMEM
FAR_OFF = pltpu.HBM


def call(kernel, in_specs, outs, scratch=(), sems=0, limit=8, table=None):
    run = pl.pallas_call(
        kernel,
        in_specs=in_specs,
        out_shape=[space(dims, dtype) for space, dims, dtype, _ in outs],
        out_specs=[spec for *_, spec in outs],
        scratch_shapes=[pltpu.VMEM(*x) for x in scratch]
        + [pltpu.SemaphoreType.DMA((sems,))] * (sems > 0)
        + ([] if table is None else [pltpu.SMEM(table.shape, table.dtype), pltpu.SemaphoreType.DMA]),
        cost_estimate=pl.CostEstimate(flops=1_000_000, bytes_accessed=1_000_000, transcendentals=0),
        compiler_params=pltpu.CompilerParams(vmem_limit_bytes=limit * MIB),
        name=kernel.__name__,
    )

    def placed(*args):
        spaces = {id(VMEM): pltpu.VMEM, id(HBM): pltpu.HBM}
        args = [
            pltpu.with_memory_space_constraint(x, spaces[id(spec)]) if id(spec) in spaces else x
            for x, spec in zip(args, in_specs)
        ]
        out = run(*args)
        return out if len(outs) > 1 else out[0]

    return placed


def body(rhs, near_blocks, near_offsets, v_factor, mix_col, mix_row, u_factor):
    count = rhs.shape[1]
    leaves = near_offsets.shape[0]
    n_row = lax.axis_size(ROW)
    n_col = lax.axis_size(COL)
    devices = n_row * n_col
    slots = leaves // n_col
    groups = leaves // 4
    width_col = n_col * RANK
    width_row = n_row * RANK
    place = near_offsets.T
    near_rows = (
        near_blocks.reshape(leaves, 4, 32, LANES).transpose(0, 2, 1, 3).reshape(leaves, LANES, LANES)
    )
    mix_first = mix_col.reshape(slots, width_col, width_col)
    mix_second = mix_row.reshape(n_col, width_row, width_row)
    field = ((RHS, count), F32)
    vc_shape = ((groups, LEAF, LANES), BF16)
    uc_shape = ((groups, RANK, 2 * LANES), BF16)
    wide_shape = ((leaves // 2, LANES, 4 * LEAF), BF16)
    z_out = (KEPT, (n_col, RHS, slots * RANK + HALO * LEAF), BF16, VMEM)
    t1_out = (KEPT, (n_row, RHS, width_col + HALO * LEAF), BF16, VMEM)
    t2_shape = ((n_col, RHS, width_row), BF16)

    def exchange(x, axes):
        return lax.all_to_all(x, axes, split_axis=0, concat_axis=0, tiled=True)

    store = ((leaves + 2 * HALO, RHS, LANES), BF16)

    vc, z, rhs_kept, mix_kept = call(
        spread_v_kernel,
        [HBM, HBM, HBM],
        [(KEPT, *vc_shape, VMEM), z_out, (KEPT, *field, VMEM), (KEPT, mix_first.shape, BF16, VMEM)],
        [(v_factor.shape, BF16)],
        16,
    )(rhs, v_factor, mix_first)

    def first_mix(z):
        return call(first_mix_kernel, [VMEM, VMEM], [t1_out])(z, mix_kept)

    z = exchange(z, COL)
    t1 = exchange(first_mix(z), ROW)
    t1, place = lax.optimization_barrier((t1, place))
    near_wide, uc, d, z = call(
        first_apply_kernel,
        [VMEM, VMEM, VMEM, VMEM, VMEM, HBM, VMEM, VMEM],
        [(KEPT, *wide_shape, VMEM), (KEPT, *uc_shape, VMEM), (KEPT, *field, VMEM), z_out],
        [field, store, store, t2_shape],
        table=place,
    )(near_rows, u_factor, rhs_kept, z, t1, place, mix_second, vc)
    z = exchange(z, COL)
    t1 = exchange(first_mix(z), ROW)
    e, sums = call(
        second_apply_kernel,
        [VMEM, VMEM, VMEM, VMEM, VMEM, HBM, VMEM, VMEM],
        [(KEPT, *field, VMEM), (KEPT, (devices, 1, 8 * RHS), F32, VMEM)],
        [field, store, store, t2_shape],
        table=place,
    )(t1, mix_second, uc, near_wide, z, place, rhs_kept, d)
    sums = exchange(sums, ROW_COL)
    return tuple(
        call(
            finish_kernel, [VMEM] * 4, [(FAR_OFF, *field, HBM)] * 2, [field, field], 8
        )(sums, rhs_kept, d, e)
    )


def solution(mesh):
    split = Mesh(mesh.devices.reshape(4, 2, 4, 4), ("row_0", "row_1", "col_0", "col_1"))
    return jax.shard_map(
        body,
        mesh=split,
        in_specs=(
            P(None, ROW_COL),
            P(ROW_COL, None, None),
            P(ROW_COL, None),
            P(ROW_COL, None),
            P(ROW, COL, None, None),
            P(ROW, COL, None, None),
            P(ROW_COL, None),
        ),
        out_specs=(P(None, ROW_COL), P(None, ROW_COL)),
        check_vma=False,
    )
```

```python
import jax
import jax.numpy as jnp
from jax import lax
from jax.experimental import pallas as pl
from jax.experimental.pallas import tpu as pltpu
from jax.sharding import Mesh
from jax.sharding import PartitionSpec as P

LEAF = 64
RANK = 32
HALO = 4
RHS = 32
LANES = 128
ROW_COL = ("row_0", "row_1", "col_0", "col_1")
ROW = ("row_0", "row_1")
COL = ("col_0", "col_1")
F32 = jnp.float32
BF16 = jnp.bfloat16


def dot(a, b):
    return jnp.dot(a, b, preferred_element_type=F32)


def dot_t(a, b):
    return lax.dot_general(a, b, (((1,), (1,)), ((), ())), preferred_element_type=F32)


def lane_group(rows):
    return lax.broadcasted_iota(jnp.int32, (rows, LANES), 1) // RANK


def lane_take(x, index):
    return jnp.take_along_axis(x, index, axis=1, mode="promise_in_bounds")


def lane_half(rows):
    return lax.broadcasted_iota(jnp.int32, (rows, LANES), 1) < LEAF


def column_index():
    return lax.axis_index("col_0") * lax.axis_size("col_1") + lax.axis_index("col_1")


def row_index():
    return lax.axis_index("row_0") * lax.axis_size("row_1") + lax.axis_index("row_1")


def pieces_of(source, target, sems, first, pieces, dim=0):
    size = source.shape[dim] // pieces
    at = [(slice(None),) * dim + (pl.ds(i * size, size),) for i in range(pieces)]
    return [pltpu.make_async_copy(source.at[x], target.at[x], sems.at[first + i]) for i, x in enumerate(at)]


class Queue:
    def __init__(self, copies, depth):
        self.copies, self.depth, self.done = copies, depth, 0
        for copy in copies[:depth]:
            copy.start()

    def wait(self, count=1):
        for _ in range(count):
            self.copies[self.done].wait()
            if self.done + self.depth < len(self.copies):
                self.copies[self.done + self.depth].start()
            self.done += 1


def wait_all(copies):
    for copy in copies:
        copy.wait()


def row_order(size, inner):
    row = lax.broadcasted_iota(jnp.int32, (size, size), 0)
    column = lax.broadcasted_iota(jnp.int32, (size, size), 1)
    outer = size // inner
    return jnp.where(column == row % outer * inner + row // outer, 1.0, 0.0).astype(BF16)


def leaf_rows(ref, sixteen, order):
    tiles = [ref[16 * sixteen : 16 * (sixteen + 1), t * LANES : (t + 1) * LANES] for t in range(16)]
    return dot(order, jnp.concatenate(tiles, axis=0))


def v_order():
    lane = lax.broadcasted_iota(jnp.int32, (RHS, LANES), 1)
    return lane // LEAF * LEAF + lane % 16 * 4 + lane % LEAF // 16


def compress(x, narrow, order, masks):
    lhs = jnp.concatenate([lane_take(x[:, t * LANES : (t + 1) * LANES], order).astype(BF16) for t in range(2)], axis=1)
    return dot(lhs, jnp.concatenate([narrow * mask for mask in masks], axis=0))


def group_masks(rows):
    group = lane_group(rows)
    return [jnp.where(group == leaf, 1.0, 0.0).astype(BF16) for leaf in range(4)]


def put_edges(v_ref, z_ref):
    n_col, _, width = z_ref.shape
    edge = HALO * LEAF
    z_ref[lax.rem(column_index() + 1, n_col), :, width - edge :] = v_ref[:, v_ref.shape[1] - edge :].astype(BF16)
    z_ref[lax.rem(column_index() + n_col - 1, n_col), :, width - edge :] = v_ref[:, :edge].astype(BF16)


def spread_v_kernel(rhs_hbm, v_hbm, mix_hbm, vc_ref, z_ref, rhs_ref, mix_ref, v_ref, sems):
    queue = Queue(pieces_of(v_hbm, v_ref, sems, 0, 4) + pieces_of(rhs_hbm, rhs_ref, sems, 4, 4, 1), 8)
    mix_in = pieces_of(mix_hbm, mix_ref, sems, 8, 8)
    for copy in mix_in:
        copy.start()
    group = lane_group(16)
    shift = column_index() % 4 * RANK
    order = row_order(256, 16)
    groups = vc_ref.shape[0]
    for sixteen in range(groups // 4):
        if sixteen % (groups // 16) == 0:
            queue.wait()
        rows = leaf_rows(v_ref, sixteen, order)
        for h in range(4):
            of_leaf = [rows[16 * leaf : 16 * (leaf + 1)] for leaf in range(4 * h, 4 * h + 4)]
            for ur in range(4):
                x = of_leaf[ur]
                for leaf in range(4):
                    if leaf != ur:
                        x = jnp.where(group == leaf, pltpu.roll(of_leaf[leaf], (leaf - ur) * RANK % LANES, 1), x)
                vc_ref[4 * sixteen + h, 16 * ur : 16 * (ur + 1), :] = x.astype(BF16)
    masks = group_masks(LEAF)
    lanes = v_order()
    for g in range(groups):
        if g % (groups // 4) == 0:
            queue.wait()
        part = compress(rhs_ref[:, 256 * g : 256 * (g + 1)], vc_ref[g], lanes, masks)
        z_ref[g // 2, :, (g % 2) * LANES : (g % 2 + 1) * LANES] = pltpu.roll(part, shift, 1).astype(BF16)
    put_edges(rhs_ref, z_ref)
    wait_all(mix_in)


def spread_u(u_ref, uc_ref):
    half = lane_half(16)
    order = row_order(256, 16)
    for sixteen in range(uc_ref.shape[0] // 4):
        rows = leaf_rows(u_ref, sixteen, order)
        for h in range(4):
            for tile in range(2):
                leaf = 4 * h + 2 * tile
                a, b = rows[16 * leaf : 16 * (leaf + 1)], rows[16 * (leaf + 1) : 16 * (leaf + 2)]
                lanes = slice(tile * LANES, (tile + 1) * LANES)
                uc_ref[4 * sixteen + h, :16, lanes] = jnp.where(half, a, pltpu.roll(b, LEAF, 1)).astype(BF16)
                uc_ref[4 * sixteen + h, 16:, lanes] = jnp.where(half, pltpu.roll(a, LEAF, 1), b).astype(BF16)


def spread_near(near_ref, out_ref):
    half = lane_half(32)
    order = row_order(LANES, 4)
    for pair in range(out_ref.shape[0]):
        both = dot(order, jnp.concatenate([near_ref[2 * pair], near_ref[2 * pair + 1]], axis=1))
        for leaf in range(2):
            block = [both[32 * b : 32 * (b + 1), leaf * LANES : (leaf + 1) * LANES] for b in range(4)]
            for h in range(2):
                first, second = block[2 * h], block[2 * h + 1]
                even = jnp.where(half, first, pltpu.roll(second, LEAF, 1))
                odd = jnp.where(half, pltpu.roll(first, LEAF, 1), second)
                lanes = slice(h * LANES, (h + 1) * LANES)
                out_ref[pair, leaf * LEAF : leaf * LEAF + 32, lanes] = even.astype(BF16)
                out_ref[pair, leaf * LEAF + 32 : leaf * LEAF + 64, lanes] = odd.astype(BF16)


def near_product(v_ref, z_ref, t1_ref, place_ref, near_ref, out_ref, held, table):
    half = lane_half(RHS)
    lane = lax.broadcasted_iota(jnp.int32, (RHS, LANES), 1)
    order = lane // LEAF * LEAF + lane % 2 * 32 + lane % LEAF // 2
    edge = HALO // 2
    tiles = v_ref.shape[1] // LANES

    def put(t, x):
        held[2 * t] = x.astype(BF16)
        held[2 * t + 1] = pltpu.roll(x, LEAF, 1).astype(BF16)

    column, row = column_index(), row_index()
    n_col, n_row = z_ref.shape[0], t1_ref.shape[0]
    z_lanes = slice(z_ref.shape[2] - HALO * LEAF, z_ref.shape[2])
    t1_lanes = slice(t1_ref.shape[2] - HALO * LEAF, t1_ref.shape[2])

    def beside(step, at_end, outside):
        near_by = z_ref[lax.clamp(0, column + step, n_col - 1), :, z_lanes].astype(F32)
        next_row = t1_ref[lax.clamp(0, row + step, n_row - 1), :, t1_lanes].astype(F32)
        return jnp.where(at_end, jnp.where(outside, 0.0, next_row), near_by)

    below = beside(-1, column == 0, row == 0)
    above = beside(1, column == n_col - 1, row == n_row - 1)
    for t in range(edge):
        put(t, below[:, t * LANES : (t + 1) * LANES])
        put(edge + tiles + t, above[:, t * LANES : (t + 1) * LANES])
    for t in range(tiles):
        put(edge + t, v_ref[:, t * LANES : (t + 1) * LANES])
    table.wait()
    for pair in range(tiles):
        lhs = [
            jnp.concatenate(
                [
                    jnp.where(
                        half,
                        held[place_ref[2 * h, leaf] + (leaf + HALO)],
                        held[(place_ref[2 * h + 1, leaf] + (leaf + HALO)) ^ 1],
                    )
                    for h in range(2)
                ],
                axis=1,
            )
            for leaf in (2 * pair, 2 * pair + 1)
        ]
        both = dot_t(jnp.concatenate(lhs, axis=0), near_ref[pair])
        out_ref[:, pair * LANES : (pair + 1) * LANES] = lane_take(jnp.where(half, both[:RHS], both[RHS:]), order)


def gather_lanes(parts, where_from, group):
    x = parts[(0 - where_from) % 4]
    for q in range(1, 4):
        x = jnp.where(group == q, parts[(q - where_from) % 4], x)
    return x


def turned_rows(ref_rows, count, where_from):
    order = [4 * four + (q - where_from) % 4 for four in range(count // 4) for q in range(4)]
    return jnp.concatenate([ref_rows[c * RANK : (c + 1) * RANK] for c in order], axis=0)


def first_mix_kernel(z_ref, mix_ref, out_ref):
    slots = mix_ref.shape[0]
    n_col = z_ref.shape[0]
    group = lane_group(RHS)
    shift = row_index() % 4 * RANK
    for j in range(slots):
        tile = j // 4
        lhs = jnp.concatenate(
            [
                gather_lanes(
                    [z_ref[4 * four + c, :, tile * LANES : (tile + 1) * LANES] for c in range(4)], j % 4, group
                )
                for four in range(n_col // 4)
            ],
            axis=1,
        )
        out = dot(lhs, turned_rows(mix_ref[j], n_col, j % 4))
        for t in range(out.shape[1] // LANES):
            out_ref[j, :, t * LANES : (t + 1) * LANES] = pltpu.roll(
                out[:, t * LANES : (t + 1) * LANES], shift, 1
            ).astype(BF16)
    first = column_index() == 0
    other_end = jnp.where(first, n_col - 1, 0)
    beside = lax.clamp(0, row_index() + jnp.where(first, 1, -1), slots - 1)
    edge = HALO * LEAF
    out_ref[beside, :, out_ref.shape[2] - edge :] = z_ref[other_end, :, z_ref.shape[2] - edge :]


def second_mix(t1_ref, mix_ref, t2_ref):
    n_row = t1_ref.shape[0]
    group = lane_group(RHS)
    count = mix_ref.shape[0]
    lane = lax.broadcasted_iota(jnp.int32, (RHS, LANES), 1)
    order = lane // RANK * RANK + lane % 16 * 2 + lane % RANK // 16
    for p in range(count):
        tile = p // 4
        lhs = jnp.concatenate(
            [
                gather_lanes(
                    [t1_ref[4 * four + r, :, tile * LANES : (tile + 1) * LANES] for r in range(4)], p % 4, group
                )
                for four in range(n_row // 4)
            ],
            axis=1,
        )
        out = dot(lhs, turned_rows(mix_ref[p], n_row, p % 4))
        for t in range(2):
            lanes = slice(t * LANES, (t + 1) * LANES)
            t2_ref[p, :, lanes] = lane_take(out[:, lanes], order).astype(BF16)


def expand_masks():
    lane = lax.broadcasted_iota(jnp.int32, (RANK, 2 * LANES), 1)
    return [jnp.where(lane // LEAF == leaf, 1.0, 0.0).astype(BF16) for leaf in range(4)]


def far_tile(t2_ref, uc_ref, masks, g):
    narrow = uc_ref[g]
    wide = jnp.concatenate([narrow * mask for mask in masks], axis=0)
    return dot(t2_ref[g // 2, :, (g % 2) * LANES : (g % 2 + 1) * LANES], wide)


def first_apply_kernel(
    rows_ref, u_ref, v_ref, in_ref, t1_ref, place_hbm, mix_ref, vc_ref,
    wide_ref, uc_ref, d_ref, z_ref,
    near_ref, held, t2_ref, place_ref, sem,
):
    table = pltpu.make_async_copy(place_hbm, place_ref, sem)
    table.start()
    spread_near(rows_ref, wide_ref)
    spread_u(u_ref, uc_ref)
    second_mix(t1_ref, mix_ref, t2_ref)
    near_product(v_ref, in_ref, t1_ref, place_ref, wide_ref, near_ref, held, table)
    shift = column_index() % 4 * RANK
    groups = uc_ref.shape[0]
    masks = expand_masks()
    for g in range(groups):
        lanes = slice(256 * g, 256 * (g + 1))
        d_ref[:, lanes] = far_tile(t2_ref, uc_ref, masks, g) + near_ref[:, lanes]
    masks = group_masks(LEAF)
    order = v_order()
    for g in range(groups):
        part = compress(d_ref[:, 256 * g : 256 * (g + 1)], vc_ref[g], order, masks)
        z_ref[g // 2, :, (g % 2) * LANES : (g % 2 + 1) * LANES] = pltpu.roll(part, shift, 1).astype(BF16)
    put_edges(d_ref, z_ref)


def second_apply_kernel(
    t1_ref, mix_ref, uc_ref, wide_ref, in_ref, place_hbm, rhs_ref, d_ref,
    e_ref, sums_ref,
    near_ref, held, t2_ref, place_ref, sem,
):
    table = pltpu.make_async_copy(place_hbm, place_ref, sem)
    table.start()
    second_mix(t1_ref, mix_ref, t2_ref)
    near_product(d_ref, in_ref, t1_ref, place_ref, wide_ref, near_ref, held, table)
    masks = expand_masks()
    total = [jnp.zeros((RHS, LANES), F32) for _ in range(6)]
    for g in range(uc_ref.shape[0]):
        wide = far_tile(t2_ref, uc_ref, masks, g) + near_ref[:, 256 * g : 256 * (g + 1)]
        e_ref[:, 256 * g : 256 * (g + 1)] = wide
        for t in range(2):
            lanes = slice(256 * g + LANES * t, 256 * g + LANES * (t + 1))
            r, d, e = rhs_ref[:, lanes], d_ref[:, lanes], wide[:, LANES * t : LANES * (t + 1)]
            terms = (r * r, r * d, d * d, r * e, d * e, e * e)
            total = [a + b for a, b in zip(total, terms)]
    stacked = jnp.concatenate(total + [jnp.zeros((2 * RHS, LANES), F32)], axis=0)
    row = jnp.sum(stacked.T, axis=0, keepdims=True)
    sums_ref[...] = jnp.broadcast_to(row[None], sums_ref.shape)


def finish_kernel(sums_ref, rhs_ref, d_ref, e_ref, solution_hbm, residual_hbm, solution_ref, residual_ref, sems):
    row = jnp.sum(sums_ref[...], axis=0)
    columns = jnp.broadcast_to(row, (LANES, row.shape[1])).T
    rr, rd, dd, re, de, ee = [columns[i * RHS : (i + 1) * RHS] for i in range(6)]
    scale = 1.0 / rr
    alpha = rd * scale
    h21_sq = (dd - alpha * rd) * scale
    h11 = 1.0 + alpha
    cross = re * scale - alpha * alpha
    inverse = 1.0 / h21_sq
    gain = ((de - alpha * dd - alpha * re + alpha * (alpha * rd)) * scale) * inverse
    h22 = 1.0 + gain
    spread = ((ee - 2.0 * alpha * de + alpha * (alpha * dd)) * scale) * inverse
    h32_sq = spread - gain * gain - cross * (cross * inverse)
    minor = h11 * h22 - cross
    determ = minor * minor + h32_sq * (h11 * h11 + h21_sq)
    x_first = (h22 * minor + h11 * h32_sq) / determ
    x_second = -minor / determ
    on_rhs = x_first - alpha * x_second
    on_d = x_first + x_second * (1.0 - alpha)
    solution_out = pieces_of(solution_ref, solution_hbm, sems, 0, 4, 1)
    residual_out = pieces_of(residual_ref, residual_hbm, sems, 4, 4, 1)
    tiles = rhs_ref.shape[1] // LANES
    for t in range(tiles):
        lanes = slice(t * LANES, (t + 1) * LANES)
        r, d, e = rhs_ref[:, lanes], d_ref[:, lanes], e_ref[:, lanes]
        solution_ref[:, lanes] = on_rhs * r + x_second * d
        residual_ref[:, lanes] = (1.0 - on_rhs) * r - on_d * d - x_second * e
        if (t + 1) % (tiles // 4) == 0:
            solution_out[t // (tiles // 4)].start()
            residual_out[t // (tiles // 4)].start()
    wait_all(solution_out + residual_out)


VMEM = pl.BlockSpec(memory_space=pltpu.VMEM)
HBM = pl.BlockSpec(memory_space=pltpu.HBM)
SMEM = pl.BlockSpec(memory_space=pltpu.SMEM)
MIB = 1 << 20
KEPT = pltpu.VMEM
FAR_OFF = pltpu.HBM


def call(kernel, in_specs, outs, scratch=(), sems=0, limit=8, table=None):
    run = pl.pallas_call(
        kernel,
        in_specs=in_specs,
        out_shape=[space(dims, dtype) for space, dims, dtype, _ in outs],
        out_specs=[spec for *_, spec in outs],
        scratch_shapes=[pltpu.VMEM(*x) for x in scratch]
        + [pltpu.SemaphoreType.DMA((sems,))] * (sems > 0)
        + ([] if table is None else [pltpu.SMEM(table.shape, table.dtype), pltpu.SemaphoreType.DMA]),
        cost_estimate=pl.CostEstimate(flops=1_000_000, bytes_accessed=1_000_000, transcendentals=0),
        compiler_params=pltpu.CompilerParams(vmem_limit_bytes=limit * MIB),
        name=kernel.__name__,
    )

    def placed(*args):
        spaces = {id(VMEM): pltpu.VMEM, id(HBM): pltpu.HBM}
        args = [
            pltpu.with_memory_space_constraint(x, spaces[id(spec)]) if id(spec) in spaces else x
            for x, spec in zip(args, in_specs)
        ]
        out = run(*args)
        return out if len(outs) > 1 else out[0]

    return placed


def body(rhs, near_blocks, near_offsets, v_factor, mix_col, mix_row, u_factor):
    count = rhs.shape[1]
    leaves = near_offsets.shape[0]
    n_row = lax.axis_size(ROW)
    n_col = lax.axis_size(COL)
    devices = n_row * n_col
    slots = leaves // n_col
    groups = leaves // 4
    width_col = n_col * RANK
    width_row = n_row * RANK
    place = near_offsets.T
    near_rows = (
        near_blocks.reshape(leaves, 4, 32, LANES).transpose(0, 2, 1, 3).reshape(leaves, LANES, LANES)
    )
    mix_first = mix_col.reshape(slots, width_col, width_col)
    mix_second = mix_row.reshape(n_col, width_row, width_row)
    field = ((RHS, count), F32)
    vc_shape = ((groups, LEAF, LANES), BF16)
    uc_shape = ((groups, RANK, 2 * LANES), BF16)
    wide_shape = ((leaves // 2, LANES, 4 * LEAF), BF16)
    z_out = (KEPT, (n_col, RHS, slots * RANK + HALO * LEAF), BF16, VMEM)
    t1_out = (KEPT, (n_row, RHS, width_col + HALO * LEAF), BF16, VMEM)
    t2_shape = ((n_col, RHS, width_row), BF16)

    def exchange(x, axes):
        return lax.all_to_all(x, axes, split_axis=0, concat_axis=0, tiled=True)

    store = ((leaves + 2 * HALO, RHS, LANES), BF16)

    vc, z, rhs_kept, mix_kept = call(
        spread_v_kernel,
        [HBM, HBM, HBM],
        [(KEPT, *vc_shape, VMEM), z_out, (KEPT, *field, VMEM), (KEPT, mix_first.shape, BF16, VMEM)],
        [(v_factor.shape, BF16)],
        16,
    )(rhs, v_factor, mix_first)

    def first_mix(z):
        return call(first_mix_kernel, [VMEM, VMEM], [t1_out])(z, mix_kept)

    z = exchange(z, COL)
    t1 = exchange(first_mix(z), ROW)
    t1, place = lax.optimization_barrier((t1, place))
    near_wide, uc, d, z = call(
        first_apply_kernel,
        [VMEM, VMEM, VMEM, VMEM, VMEM, HBM, VMEM, VMEM],
        [(KEPT, *wide_shape, VMEM), (KEPT, *uc_shape, VMEM), (KEPT, *field, VMEM), z_out],
        [field, store, t2_shape],
        table=place,
    )(near_rows, u_factor, rhs_kept, z, t1, place, mix_second, vc)
    z = exchange(z, COL)
    t1 = exchange(first_mix(z), ROW)
    e, sums = call(
        second_apply_kernel,
        [VMEM, VMEM, VMEM, VMEM, VMEM, HBM, VMEM, VMEM],
        [(KEPT, *field, VMEM), (KEPT, (devices, 1, 8 * RHS), F32, VMEM)],
        [field, store, t2_shape],
        table=place,
    )(t1, mix_second, uc, near_wide, z, place, rhs_kept, d)
    sums = exchange(sums, ROW_COL)
    return tuple(
        call(
            finish_kernel, [VMEM] * 4, [(FAR_OFF, *field, HBM)] * 2, [field, field], 8
        )(sums, rhs_kept, d, e)
    )


def solution(mesh):
    split = Mesh(mesh.devices.reshape(4, 2, 4, 4), ("row_0", "row_1", "col_0", "col_1"))
    return jax.shard_map(
        body,
        mesh=split,
        in_specs=(
            P(None, ROW_COL),
            P(ROW_COL, None, None),
            P(ROW_COL, None),
            P(ROW_COL, None),
            P(ROW, COL, None, None),
            P(ROW, COL, None, None),
            P(ROW_COL, None),
        ),
        out_specs=(P(None, ROW_COL), P(None, ROW_COL)),
        check_vma=False,
    )
```

```python
import jax
import jax.numpy as jnp
from jax import lax
from jax.experimental import pallas as pl
from jax.experimental.pallas import tpu as pltpu
from jax.sharding import Mesh
from jax.sharding import PartitionSpec as P

LEAF = 64
RANK = 32
HALO = 4
RHS = 32
LANES = 128
ROW_COL = ("row_0", "row_1", "col_0", "col_1")
ROW = ("row_0", "row_1")
COL = ("col_0", "col_1")
F32 = jnp.float32
BF16 = jnp.bfloat16


def dot(a, b):
    return jnp.dot(a, b, preferred_element_type=F32)


def dot_t(a, b):
    return lax.dot_general(a, b, (((1,), (1,)), ((), ())), preferred_element_type=F32)


def lane_group(rows):
    return lax.broadcasted_iota(jnp.int32, (rows, LANES), 1) // RANK


def lane_take(x, index):
    return jnp.take_along_axis(x, index, axis=1, mode="promise_in_bounds")


def lane_half(rows):
    return lax.broadcasted_iota(jnp.int32, (rows, LANES), 1) < LEAF


def column_index():
    return lax.axis_index("col_0") * lax.axis_size("col_1") + lax.axis_index("col_1")


def row_index():
    return lax.axis_index("row_0") * lax.axis_size("row_1") + lax.axis_index("row_1")


def pieces_of(source, target, sems, first, pieces, dim=0):
    size = source.shape[dim] // pieces
    at = [(slice(None),) * dim + (pl.ds(i * size, size),) for i in range(pieces)]
    return [pltpu.make_async_copy(source.at[x], target.at[x], sems.at[first + i]) for i, x in enumerate(at)]


class Queue:
    def __init__(self, copies, depth):
        self.copies, self.depth, self.done = copies, depth, 0
        for copy in copies[:depth]:
            copy.start()

    def wait(self, count=1):
        for _ in range(count):
            self.copies[self.done].wait()
            if self.done + self.depth < len(self.copies):
                self.copies[self.done + self.depth].start()
            self.done += 1


def wait_all(copies):
    for copy in copies:
        copy.wait()


def row_order(size, inner):
    row = lax.broadcasted_iota(jnp.int32, (size, size), 0)
    column = lax.broadcasted_iota(jnp.int32, (size, size), 1)
    outer = size // inner
    return jnp.where(column == row % outer * inner + row // outer, 1.0, 0.0).astype(BF16)


def leaf_rows(ref, sixteen, order):
    tiles = [ref[16 * sixteen : 16 * (sixteen + 1), t * LANES : (t + 1) * LANES] for t in range(16)]
    return dot(order, jnp.concatenate(tiles, axis=0))


def v_order():
    lane = lax.broadcasted_iota(jnp.int32, (RHS, LANES), 1)
    return lane // LEAF * LEAF + lane % 16 * 4 + lane % LEAF // 16


def compress(x, narrow, order, masks):
    lhs = jnp.concatenate([lane_take(x[:, t * LANES : (t + 1) * LANES], order).astype(BF16) for t in range(2)], axis=1)
    return dot(lhs, jnp.concatenate([narrow * mask for mask in masks], axis=0))


def group_masks(rows):
    group = lane_group(rows)
    return [jnp.where(group == leaf, 1.0, 0.0).astype(BF16) for leaf in range(4)]


def put_edges(v_ref, z_ref):
    n_col, _, width = z_ref.shape
    edge = HALO * LEAF
    z_ref[lax.rem(column_index() + 1, n_col), :, width - edge :] = v_ref[:, v_ref.shape[1] - edge :].astype(BF16)
    z_ref[lax.rem(column_index() + n_col - 1, n_col), :, width - edge :] = v_ref[:, :edge].astype(BF16)


def spread_v_kernel(rhs_hbm, v_hbm, vc_ref, z_ref, rhs_ref, v_ref, sems):
    queue = Queue(pieces_of(v_hbm, v_ref, sems, 0, 4) + pieces_of(rhs_hbm, rhs_ref, sems, 4, 4, 1), 8)
    group = lane_group(16)
    shift = column_index() % 4 * RANK
    order = row_order(256, 16)
    groups = vc_ref.shape[0]
    masks = group_masks(LEAF)
    lanes = v_order()
    queue.wait(8)
    for sixteen in range(groups // 4):
        rows = leaf_rows(v_ref, sixteen, order)
        for h in range(4):
            g = 4 * sixteen + h
            of_leaf = [rows[16 * leaf : 16 * (leaf + 1)] for leaf in range(4 * h, 4 * h + 4)]
            narrow = []
            for ur in range(4):
                x = of_leaf[ur]
                for leaf in range(4):
                    if leaf != ur:
                        x = jnp.where(group == leaf, pltpu.roll(of_leaf[leaf], (leaf - ur) * RANK % LANES, 1), x)
                narrow.append(x.astype(BF16))
            narrow = jnp.concatenate(narrow, axis=0)
            vc_ref[g] = narrow
            part = compress(rhs_ref[:, 256 * g : 256 * (g + 1)], narrow, lanes, masks)
            z_ref[g // 2, :, (g % 2) * LANES : (g % 2 + 1) * LANES] = pltpu.roll(part, shift, 1).astype(BF16)


def edges_kernel(rhs_ref, z_in_ref, z_ref):
    put_edges(rhs_ref, z_ref)


def spread_u(u_ref, uc_ref):
    half = lane_half(16)
    order = row_order(256, 16)
    for sixteen in range(uc_ref.shape[0] // 4):
        rows = leaf_rows(u_ref, sixteen, order)
        for h in range(4):
            for tile in range(2):
                leaf = 4 * h + 2 * tile
                a, b = rows[16 * leaf : 16 * (leaf + 1)], rows[16 * (leaf + 1) : 16 * (leaf + 2)]
                lanes = slice(tile * LANES, (tile + 1) * LANES)
                uc_ref[4 * sixteen + h, :16, lanes] = jnp.where(half, a, pltpu.roll(b, LEAF, 1)).astype(BF16)
                uc_ref[4 * sixteen + h, 16:, lanes] = jnp.where(half, pltpu.roll(a, LEAF, 1), b).astype(BF16)


def spread_near(near_ref, out_ref):
    half = lane_half(32)
    order = row_order(LANES, 4)
    for pair in range(out_ref.shape[0]):
        both = dot(order, jnp.concatenate([near_ref[2 * pair], near_ref[2 * pair + 1]], axis=1))
        for leaf in range(2):
            block = [both[32 * b : 32 * (b + 1), leaf * LANES : (leaf + 1) * LANES] for b in range(4)]
            for h in range(2):
                first, second = block[2 * h], block[2 * h + 1]
                even = jnp.where(half, first, pltpu.roll(second, LEAF, 1))
                odd = jnp.where(half, pltpu.roll(first, LEAF, 1), second)
                lanes = slice(h * LANES, (h + 1) * LANES)
                out_ref[pair, leaf * LEAF : leaf * LEAF + 32, lanes] = even.astype(BF16)
                out_ref[pair, leaf * LEAF + 32 : leaf * LEAF + 64, lanes] = odd.astype(BF16)


def near_product(v_ref, z_ref, t1_ref, place_ref, near_ref, out_ref, held, table):
    half = lane_half(RHS)
    lane = lax.broadcasted_iota(jnp.int32, (RHS, LANES), 1)
    order = lane // LEAF * LEAF + lane % 2 * 32 + lane % LEAF // 2
    edge = HALO // 2
    tiles = v_ref.shape[1] // LANES

    def put(t, x):
        held[2 * t] = x.astype(BF16)
        held[2 * t + 1] = pltpu.roll(x, LEAF, 1).astype(BF16)

    column, row = column_index(), row_index()
    n_col, n_row = z_ref.shape[0], t1_ref.shape[0]
    z_lanes = slice(z_ref.shape[2] - HALO * LEAF, z_ref.shape[2])
    t1_lanes = slice(t1_ref.shape[2] - HALO * LEAF, t1_ref.shape[2])

    def beside(step, at_end, outside):
        near_by = z_ref[lax.clamp(0, column + step, n_col - 1), :, z_lanes].astype(F32)
        next_row = t1_ref[lax.clamp(0, row + step, n_row - 1), :, t1_lanes].astype(F32)
        return jnp.where(at_end, jnp.where(outside, 0.0, next_row), near_by)

    below = beside(-1, column == 0, row == 0)
    above = beside(1, column == n_col - 1, row == n_row - 1)
    for t in range(edge):
        put(t, below[:, t * LANES : (t + 1) * LANES])
        put(edge + tiles + t, above[:, t * LANES : (t + 1) * LANES])
    for t in range(tiles):
        put(edge + t, v_ref[:, t * LANES : (t + 1) * LANES])
    table.wait()
    for pair in range(tiles):
        lhs = [
            jnp.concatenate(
                [
                    jnp.where(
                        half,
                        held[place_ref[2 * h, leaf] + (leaf + HALO)],
                        held[(place_ref[2 * h + 1, leaf] + (leaf + HALO)) ^ 1],
                    )
                    for h in range(2)
                ],
                axis=1,
            )
            for leaf in (2 * pair, 2 * pair + 1)
        ]
        both = dot_t(jnp.concatenate(lhs, axis=0), near_ref[pair])
        out_ref[:, pair * LANES : (pair + 1) * LANES] = lane_take(jnp.where(half, both[:RHS], both[RHS:]), order)


def gather_lanes(parts, where_from, group):
    x = parts[(0 - where_from) % 4]
    for q in range(1, 4):
        x = jnp.where(group == q, parts[(q - where_from) % 4], x)
    return x


def turned_rows(ref_rows, count, where_from):
    order = [4 * four + (q - where_from) % 4 for four in range(count // 4) for q in range(4)]
    return jnp.concatenate([ref_rows[c * RANK : (c + 1) * RANK] for c in order], axis=0)


def first_mix_kernel(z_ref, mix_ref, out_ref):
    slots = mix_ref.shape[0]
    n_col = z_ref.shape[0]
    group = lane_group(RHS)
    shift = row_index() % 4 * RANK
    for j in range(slots):
        tile = j // 4
        lhs = jnp.concatenate(
            [
                gather_lanes(
                    [z_ref[4 * four + c, :, tile * LANES : (tile + 1) * LANES] for c in range(4)], j % 4, group
                )
                for four in range(n_col // 4)
            ],
            axis=1,
        )
        out = dot(lhs, turned_rows(mix_ref[j], n_col, j % 4))
        for t in range(out.shape[1] // LANES):
            out_ref[j, :, t * LANES : (t + 1) * LANES] = pltpu.roll(
                out[:, t * LANES : (t + 1) * LANES], shift, 1
            ).astype(BF16)
    first = column_index() == 0
    other_end = jnp.where(first, n_col - 1, 0)
    beside = lax.clamp(0, row_index() + jnp.where(first, 1, -1), slots - 1)
    edge = HALO * LEAF
    out_ref[beside, :, out_ref.shape[2] - edge :] = z_ref[other_end, :, z_ref.shape[2] - edge :]


def second_mix(t1_ref, mix_ref, t2_ref):
    n_row = t1_ref.shape[0]
    group = lane_group(RHS)
    count = mix_ref.shape[0]
    lane = lax.broadcasted_iota(jnp.int32, (RHS, LANES), 1)
    order = lane // RANK * RANK + lane % 16 * 2 + lane % RANK // 16
    for p in range(count):
        tile = p // 4
        lhs = jnp.concatenate(
            [
                gather_lanes(
                    [t1_ref[4 * four + r, :, tile * LANES : (tile + 1) * LANES] for r in range(4)], p % 4, group
                )
                for four in range(n_row // 4)
            ],
            axis=1,
        )
        out = dot(lhs, turned_rows(mix_ref[p], n_row, p % 4))
        for t in range(2):
            lanes = slice(t * LANES, (t + 1) * LANES)
            t2_ref[p, :, lanes] = lane_take(out[:, lanes], order).astype(BF16)


def expand_masks():
    lane = lax.broadcasted_iota(jnp.int32, (RANK, 2 * LANES), 1)
    return [jnp.where(lane // LEAF == leaf, 1.0, 0.0).astype(BF16) for leaf in range(4)]


def far_tile(t2_ref, uc_ref, masks, g):
    narrow = uc_ref[g]
    wide = jnp.concatenate([narrow * mask for mask in masks], axis=0)
    return dot(t2_ref[g // 2, :, (g % 2) * LANES : (g % 2 + 1) * LANES], wide)


def first_apply_kernel(
    rows_ref, u_ref, v_ref, in_ref, t1_ref, place_hbm, mix_ref, vc_ref,
    wide_ref, uc_ref, d_ref, z_ref,
    near_ref, held, t2_ref, place_ref, sem,
):
    table = pltpu.make_async_copy(place_hbm, place_ref, sem)
    table.start()
    spread_near(rows_ref, wide_ref)
    spread_u(u_ref, uc_ref)
    second_mix(t1_ref, mix_ref, t2_ref)
    near_product(v_ref, in_ref, t1_ref, place_ref, wide_ref, near_ref, held, table)
    shift = column_index() % 4 * RANK
    groups = uc_ref.shape[0]
    masks = expand_masks()
    for g in range(groups):
        lanes = slice(256 * g, 256 * (g + 1))
        d_ref[:, lanes] = far_tile(t2_ref, uc_ref, masks, g) + near_ref[:, lanes]
    masks = group_masks(LEAF)
    order = v_order()
    for g in range(groups):
        part = compress(d_ref[:, 256 * g : 256 * (g + 1)], vc_ref[g], order, masks)
        z_ref[g // 2, :, (g % 2) * LANES : (g % 2 + 1) * LANES] = pltpu.roll(part, shift, 1).astype(BF16)
    put_edges(d_ref, z_ref)


def second_apply_kernel(
    t1_ref, mix_ref, uc_ref, wide_ref, in_ref, place_hbm, rhs_ref, d_ref,
    e_ref, sums_ref,
    near_ref, held, t2_ref, place_ref, sem,
):
    table = pltpu.make_async_copy(place_hbm, place_ref, sem)
    table.start()
    second_mix(t1_ref, mix_ref, t2_ref)
    near_product(d_ref, in_ref, t1_ref, place_ref, wide_ref, near_ref, held, table)
    masks = expand_masks()
    total = [jnp.zeros((RHS, LANES), F32) for _ in range(6)]
    for g in range(uc_ref.shape[0]):
        wide = far_tile(t2_ref, uc_ref, masks, g) + near_ref[:, 256 * g : 256 * (g + 1)]
        e_ref[:, 256 * g : 256 * (g + 1)] = wide
        for t in range(2):
            lanes = slice(256 * g + LANES * t, 256 * g + LANES * (t + 1))
            r, d, e = rhs_ref[:, lanes], d_ref[:, lanes], wide[:, LANES * t : LANES * (t + 1)]
            terms = (r * r, r * d, d * d, r * e, d * e, e * e)
            total = [a + b for a, b in zip(total, terms)]
    stacked = jnp.concatenate(total + [jnp.zeros((2 * RHS, LANES), F32)], axis=0)
    row = jnp.sum(stacked.T, axis=0, keepdims=True)
    sums_ref[...] = jnp.broadcast_to(row[None], sums_ref.shape)


def finish_kernel(sums_ref, rhs_ref, d_ref, e_ref, solution_hbm, residual_hbm, solution_ref, residual_ref, sems):
    row = jnp.sum(sums_ref[...], axis=0)
    columns = jnp.broadcast_to(row, (LANES, row.shape[1])).T
    rr, rd, dd, re, de, ee = [columns[i * RHS : (i + 1) * RHS] for i in range(6)]
    scale = 1.0 / rr
    alpha = rd * scale
    h21_sq = (dd - alpha * rd) * scale
    h11 = 1.0 + alpha
    cross = re * scale - alpha * alpha
    inverse = 1.0 / h21_sq
    gain = ((de - alpha * dd - alpha * re + alpha * (alpha * rd)) * scale) * inverse
    h22 = 1.0 + gain
    spread = ((ee - 2.0 * alpha * de + alpha * (alpha * dd)) * scale) * inverse
    h32_sq = spread - gain * gain - cross * (cross * inverse)
    minor = h11 * h22 - cross
    determ = minor * minor + h32_sq * (h11 * h11 + h21_sq)
    x_first = (h22 * minor + h11 * h32_sq) / determ
    x_second = -minor / determ
    on_rhs = x_first - alpha * x_second
    on_d = x_first + x_second * (1.0 - alpha)
    solution_out = pieces_of(solution_ref, solution_hbm, sems, 0, 4, 1)
    residual_out = pieces_of(residual_ref, residual_hbm, sems, 4, 4, 1)
    tiles = rhs_ref.shape[1] // LANES
    for t in range(tiles):
        lanes = slice(t * LANES, (t + 1) * LANES)
        r, d, e = rhs_ref[:, lanes], d_ref[:, lanes], e_ref[:, lanes]
        solution_ref[:, lanes] = on_rhs * r + x_second * d
        residual_ref[:, lanes] = (1.0 - on_rhs) * r - on_d * d - x_second * e
        if (t + 1) % (tiles // 4) == 0:
            solution_out[t // (tiles // 4)].start()
            residual_out[t // (tiles // 4)].start()
    wait_all(solution_out + residual_out)


VMEM = pl.BlockSpec(memory_space=pltpu.VMEM)
HBM = pl.BlockSpec(memory_space=pltpu.HBM)
SMEM = pl.BlockSpec(memory_space=pltpu.SMEM)
MIB = 1 << 20
KEPT = pltpu.VMEM
FAR_OFF = pltpu.HBM


def call(kernel, in_specs, outs, scratch=(), sems=0, limit=8, table=None, flops=1_000_000, aliases=None):
    run = pl.pallas_call(
        kernel,
        in_specs=in_specs,
        out_shape=[space(dims, dtype) for space, dims, dtype, _ in outs],
        out_specs=[spec for *_, spec in outs],
        scratch_shapes=[pltpu.VMEM(*x) for x in scratch]
        + [pltpu.SemaphoreType.DMA((sems,))] * (sems > 0)
        + ([] if table is None else [pltpu.SMEM(table.shape, table.dtype), pltpu.SemaphoreType.DMA]),
        cost_estimate=pl.CostEstimate(flops=flops, bytes_accessed=max(1_000_000, flops // 1000), transcendentals=0),
        input_output_aliases=aliases or {},
        compiler_params=pltpu.CompilerParams(vmem_limit_bytes=limit * MIB),
        name=kernel.__name__,
    )

    def placed(*args):
        spaces = {id(VMEM): pltpu.VMEM, id(HBM): pltpu.HBM}
        args = [
            pltpu.with_memory_space_constraint(x, spaces[id(spec)]) if id(spec) in spaces else x
            for x, spec in zip(args, in_specs)
        ]
        out = run(*args)
        return out if len(outs) > 1 else out[0]

    return placed


def body(rhs, near_blocks, near_offsets, v_factor, mix_col, mix_row, u_factor):
    count = rhs.shape[1]
    leaves = near_offsets.shape[0]
    n_row = lax.axis_size(ROW)
    n_col = lax.axis_size(COL)
    devices = n_row * n_col
    slots = leaves // n_col
    groups = leaves // 4
    width_col = n_col * RANK
    width_row = n_row * RANK
    place = near_offsets.T
    near_rows = (
        near_blocks.reshape(leaves, 4, 32, LANES).transpose(0, 2, 1, 3).reshape(leaves, LANES, LANES)
    )
    mix_first = mix_col.reshape(slots, width_col, width_col)
    mix_second = mix_row.reshape(n_col, width_row, width_row)
    field = ((RHS, count), F32)
    vc_shape = ((groups, LEAF, LANES), BF16)
    uc_shape = ((groups, RANK, 2 * LANES), BF16)
    wide_shape = ((leaves // 2, LANES, 4 * LEAF), BF16)
    z_out = (KEPT, (n_col, RHS, slots * RANK + HALO * LEAF), BF16, VMEM)
    t1_out = (KEPT, (n_row, RHS, width_col + HALO * LEAF), BF16, VMEM)
    t2_shape = ((n_col, RHS, width_row), BF16)

    def exchange(x, axes):
        return lax.all_to_all(x, axes, split_axis=0, concat_axis=0, tiled=True)

    store = ((leaves + 2 * HALO, RHS, LANES), BF16)

    vc, z, rhs_kept = call(
        spread_v_kernel,
        [HBM, HBM],
        [(KEPT, *vc_shape, VMEM), z_out, (KEPT, *field, VMEM)],
        [(v_factor.shape, BF16)],
        8,
    )(rhs, v_factor)
    z = call(edges_kernel, [VMEM, VMEM], [z_out], flops=20_000_000_000, aliases={1: 0})(rhs_kept, z)

    def first_mix(z):
        return call(first_mix_kernel, [VMEM, VMEM], [t1_out])(z, mix_first)

    z = exchange(z, COL)
    t1 = exchange(first_mix(z), ROW)
    t1, place = lax.optimization_barrier((t1, place))
    near_wide, uc, d, z = call(
        first_apply_kernel,
        [VMEM, VMEM, VMEM, VMEM, VMEM, HBM, VMEM, VMEM],
        [(KEPT, *wide_shape, VMEM), (KEPT, *uc_shape, VMEM), (KEPT, *field, VMEM), z_out],
        [field, store, t2_shape],
        table=place,
    )(near_rows, u_factor, rhs_kept, z, t1, place, mix_second, vc)
    z = exchange(z, COL)
    t1 = exchange(first_mix(z), ROW)
    e, sums = call(
        second_apply_kernel,
        [VMEM, VMEM, VMEM, VMEM, VMEM, HBM, VMEM, VMEM],
        [(KEPT, *field, VMEM), (KEPT, (devices, 1, 8 * RHS), F32, VMEM)],
        [field, store, t2_shape],
        table=place,
    )(t1, mix_second, uc, near_wide, z, place, rhs_kept, d)
    sums = exchange(sums, ROW_COL)
    return tuple(
        call(
            finish_kernel, [VMEM] * 4, [(FAR_OFF, *field, HBM)] * 2, [field, field], 8
        )(sums, rhs_kept, d, e)
    )


def solution(mesh):
    split = Mesh(mesh.devices.reshape(4, 2, 4, 4), ("row_0", "row_1", "col_0", "col_1"))
    return jax.shard_map(
        body,
        mesh=split,
        in_specs=(
            P(None, ROW_COL),
            P(ROW_COL, None, None),
            P(ROW_COL, None),
            P(ROW_COL, None),
            P(ROW, COL, None, None),
            P(ROW, COL, None, None),
            P(ROW_COL, None),
        ),
        out_specs=(P(None, ROW_COL), P(None, ROW_COL)),
        check_vma=False,
    )
```
